32 devices in a mesh: parts: 2 (over x), expert: 16 (over z, y, core).
Axes of the slice: x: 2, y: 2, z: 4, core: 2. Of those that a mesh axis runs over, the one named last changes fastest.
Arguments:
- tokens: bfloat16 [2, 128, 7168], P(None, ('parts', 'expert')), parts along dimension 1, may hold values from -6 to 6
- live_rows: int32 [2, 32], P(None, ('parts', 'expert')), parts along dimension 1, may hold values from 3 to 4
- expert_ids: int32 [1, 2, 128, 8], P(None, None, ('parts', 'expert')), parts along dimension 2, may hold values from 0 to 15, all different within a row; in each aligned block of 4 rows (0 to 3, 4 to 7, ..., all dimensions but the last counted through in order) at most 2 rows name the same one
- gate_weights: float32 [1, 2, 128, 8], P(None, None, ('parts', 'expert')), parts along dimension 2, may hold values from 0.25 to 2.5
- norm_gain: float32 [1, 7168], replicated, may hold values from 0.1 to 1.9
- expert_gate_up: bfloat16 [1, 16, 7168, 2048], P(None, 'expert'), may hold values from -0.0625 to 0.0625
- expert_down: bfloat16 [1, 16, 1024, 7168], P(None, 'expert'), may hold values from -0.1875 to 0.1875
- shared_gate_up: bfloat16 [1, 7168, 2048], P(None, 'expert'), may hold values from -0.0625 to 0.0625
- shared_down: bfloat16 [1, 1024, 7168], P(None, None, 'expert'), may hold values from -0.1875 to 0.1875
Outputs:
- hidden_out: bfloat16 [2, 128, 7168], P(None, ('parts', 'expert')), parts along dimension 1
The draws below stay inside these ranges and needn't reach their ends.
There are 2 independent parts, one for each index of `parts`. The reference program is written for one: setup_inputs(seed, part) draws one part's arguments, and reference() takes and returns one part's arrays. A program takes and returns all parts, laid end to end along the dimension named above; an argument that names none is the same for every part. Nothing has to cross between parts.
Inputs may be any that keep to these rules, and one draw needn't show every extreme that they name: `expert_ids`: the 8 ids of a row differ; within the rows of one device for one layer and step, no expert is named by more than 2 rows, a bound that some block reaches.
All inputs are finite; a program needn't handle non-finite values.
Results may differ from the reference program's by a relative error of at most 0.0068.
Values may be sent and summed in bfloat16 or wider, within the bound.
A program may use at most 128 MiB of HBM per device.

```python
import math
import jax
import jax.numpy as jnp
import numpy as np
from jax import lax

D = 7168
TOP = 8
HID = 1024
SHARED = 1024
EXPERTS = 16
LAYERS = 1
STEPS = 2
ROWS_DEV = 4
GROUP = 1
TOKENS = 64
CAP = 2
N_EXPERT = 16


def with_ends(values, own_key, least, top_value):
    index_at = [jax.random.randint(jax.random.fold_in(own_key, axis), (), 0, length) for axis, length in enumerate(values.shape)]
    longest = values.shape.index(max(values.shape))
    beside = index_at[:longest] + [(index_at[longest] + 1) % values.shape[longest]] + index_at[longest + 1:]
    return values.at[tuple(index_at)].set(least).at[tuple(beside)].set(top_value)


def levels(own_key, shape, shards, low, top_value):
    gain, own = 1.0, jax.random.fold_in(own_key, 6)
    for axis_at, shards_of in shards:
        heights = jnp.exp(jax.random.uniform(jax.random.fold_in(own, axis_at), (shards_of,), jnp.float32, low / len(shards), top_value / len(shards)))
        gain = gain * jnp.repeat(heights, shape[axis_at] // shards_of).reshape([-1 if axis == axis_at else 1 for axis in range(len(shape))])
    return gain


def deal_out(stream_key, own, number, rows, number_of, top, most, lean):
    sequence = jax.random.permutation(stream_key, number_of)
    packed, common = shares(number_of, rows * top, most, lean, True), shares(number_of, rows * top, most, lean, False)
    places = jnp.arange(number_of)

    def named(sizes, rotation):
        used = int((sizes > 0).sum())
        fixed = max(1, used // 4)
        shifted = fixed + (places - fixed + rotation * (used - fixed)) % max(1, number_of - fixed)
        return jnp.zeros((number_of,), jnp.int32).at[sequence[jnp.where(places < fixed, places, shifted)]].set(jnp.asarray(sizes, jnp.int32))

    sizes = jnp.where(number % 4 == 0, named(packed, number // 4), named(common, number - number // 4 - 1))
    mixed = jax.random.permutation(jax.random.fold_in(own, 3), number_of)
    donor, taker = mixed[0:number_of // 2 * 2:2], mixed[1:number_of // 2 * 2:2]
    room = jnp.minimum(sizes[donor] - 1, most - sizes[taker]) // 2
    room = jnp.where((donor == sequence[0]) | (taker == sequence[0]) | (sizes[taker] == 0), 0, jnp.maximum(room, 0))
    shifted = jax.random.randint(jax.random.fold_in(own, 4), (number_of // 2,), 0, 1 << 20) % (room + 1)
    sizes = sizes.at[donor].add(-shifted).at[taker].add(shifted)
    items = jnp.searchsorted(jnp.cumsum(sizes), jnp.arange(rows * top), side="right").astype(jnp.int32)
    table = items.reshape(top, rows).T
    table = table[jax.random.permutation(jax.random.fold_in(own, 1), rows)]
    rotation = jax.random.randint(jax.random.fold_in(own, 2), (rows, 1), 0, top)
    return jnp.take_along_axis(table, (jnp.arange(top)[None, :] + rotation) % top, axis=1)


def shares(count, total, most, lean, full):
    loads = [(1 << 20) // math.isqrt(rank ** lean) + 1 for rank in range(1, count + 1)]
    largest = most if full else min(most, max(-(-total // count), total * loads[0] // sum(loads)))
    least = 1 if total - largest >= count - 1 else 0
    given, surplus = [largest] + [least] * (count - 1), total - largest - least * (count - 1)
    while surplus > 0:
        candidates = [i for i in range(1, count) if given[i] < largest] or [i for i in range(1, count) if given[i] < most]
        mass, left = sum([loads[i] for i in candidates]), surplus
        for i in candidates:
            more = min(most - given[i], max(1, left * loads[i] // mass), surplus)
            given[i] = given[i] + more
            surplus = surplus - more
    return np.array(given)


def centred(key, extent, spread, bound, shards=(), held_as=jnp.bfloat16):
    entries = spread * jax.random.normal(key, extent, jnp.float32)
    if shards:
        entries = entries * levels(key, extent, shards, -0.22, 0.18)
    return jnp.clip(entries, -bound, bound).astype(held_as)


def setup_inputs(seed: int = 0, part: int = 0) -> dict:
    arg_keys = jax.random.split(jax.random.key(seed), 10)
    part_splits = jax.random.split(jax.random.fold_in(arg_keys[9], part), 10)
    tokens = centred(part_splits[0], (STEPS, TOKENS, D), 1.0, 6.0, ((1, 16),))
    live_rows = with_ends(jax.random.randint(part_splits[1], (STEPS, N_EXPERT), (3 * ROWS_DEV) // 4, ROWS_DEV + 1), jax.random.fold_in(part_splits[1], 1), (3 * ROWS_DEV) // 4, ROWS_DEV).astype(jnp.int32)
    expert_ids_keys = jax.random.split(jax.random.fold_in(part_splits[2], 1), LAYERS * STEPS * TOKENS // ROWS_DEV)
    expert_ids_turns = jax.random.permutation(jax.random.fold_in(part_splits[2], 3), LAYERS * STEPS * TOKENS // ROWS_DEV)
    expert_ids = jax.vmap(lambda own, number: deal_out(jax.random.fold_in(part_splits[2], 2), own, number, ROWS_DEV, EXPERTS, TOP, CAP, 2))(expert_ids_keys, expert_ids_turns).reshape((LAYERS, STEPS, TOKENS, TOP))
    gate_weights = jnp.clip(jnp.exp(math.log(2.5) - 2.3025851 * jax.random.uniform(part_splits[3], (LAYERS, STEPS, TOKENS, TOP), jnp.float32) ** levels(part_splits[3], (LAYERS, STEPS, TOKENS, TOP), ((2, 16),), -0.2, 0.2)), 0.25, 2.5)
    norm_gain = jnp.clip(1.0 + 0.18 * jax.random.normal(arg_keys[4], (LAYERS, D), jnp.float32), 0.1, 1.9)
    expert_gate_up = centred(arg_keys[5], (LAYERS, EXPERTS * GROUP, D, 2 * HID // GROUP), D ** -0.5, 0.0625, ((1, 16),))
    expert_down = centred(arg_keys[6], (LAYERS, EXPERTS * GROUP, HID // GROUP, D), HID ** -0.5, 0.1875, ((1, 16),))
    shared_gate_up = centred(arg_keys[7], (LAYERS, D, 2 * SHARED), D ** -0.5, 0.0625, ((1, 16),))
    shared_down = centred(arg_keys[8], (LAYERS, SHARED, D), SHARED ** -0.5, 0.1875, ((2, 16),))
    return {"tokens": tokens, "live_rows": live_rows, "expert_ids": expert_ids, "gate_weights": gate_weights, "norm_gain": norm_gain, "expert_gate_up": expert_gate_up, "expert_down": expert_down, "shared_gate_up": shared_gate_up, "shared_down": shared_down}


EPSILON = 1e-06

def rms_normed(hidden, gain_row):
    widened = hidden.astype(jnp.float32)
    scaling = lax.rsqrt(lax.optimization_barrier(jnp.mean(widened * widened, axis=-1, keepdims=True)) + EPSILON)
    return (widened * scaling * gain_row).astype(jnp.bfloat16)

def swiglu(inputs, gate_up, down_proj, unit_count):
    projected = jnp.dot(inputs, gate_up, preferred_element_type=jnp.float32)
    activated = (jax.nn.silu(projected[:, :unit_count]) * projected[:, unit_count:]).astype(jnp.bfloat16)
    return jnp.dot(activated, down_proj, preferred_element_type=jnp.float32).astype(jnp.bfloat16)

def partial_swiglu(inputs, gate_up, down_proj, unit_count):
    projected = jnp.dot(inputs, gate_up, preferred_element_type=jnp.float32)
    activated = (jax.nn.silu(projected[:, :unit_count]) * projected[:, unit_count:]).astype(jnp.bfloat16)
    return jnp.dot(activated, down_proj, preferred_element_type=jnp.float32)

def routed_sum(normed, id_block, gate_block, is_live, gate_up, down_proj):
    unit_block = HID // GROUP
    grouped_up = gate_up.reshape(EXPERTS, GROUP, D, 2 * unit_block)
    grouped_down = down_proj.reshape(EXPERTS, GROUP, unit_block, D)
    flat_ids = jnp.where(is_live[:, None], id_block, -1).reshape(-1)
    flat_gates = gate_block.reshape(-1)
    slot_count = N_EXPERT * CAP

    def one_expert(carry_sum, expert):
        hit_mask = (flat_ids == expert).astype(jnp.int32)
        ordering = jnp.argsort(-hit_mask, stable=True)[:slot_count]
        picked = hit_mask[ordering].astype(jnp.float32)
        row_index = (ordering // TOP).astype(jnp.int32)
        chosen = normed[row_index]
        upper = grouped_up[expert]
        lower = grouped_down[expert]
        total = jnp.zeros((slot_count, D), jnp.float32)
        for member in range(GROUP):
            total = total + partial_swiglu(chosen, upper[member], lower[member], unit_block)
        outputs = total.astype(jnp.bfloat16)
        weighted = (flat_gates[ordering] * picked)[:, None] * outputs.astype(jnp.float32)
        return (carry_sum.at[row_index].add(weighted), None)
    start_sum = jnp.zeros((TOKENS, D), jnp.float32)
    final_sum, _ = lax.scan(one_expert, start_sum, jnp.arange(EXPERTS, dtype=jnp.int32))
    return final_sum

def reference(tokens, live_rows, expert_ids, gate_weights, norm_gain, expert_gate_up, expert_down, shared_gate_up, shared_down):
    position = jnp.arange(TOKENS, dtype=jnp.int32)
    results = []
    for step_at in range(STEPS):
        is_live = position % ROWS_DEV < jnp.repeat(live_rows[step_at], ROWS_DEV)
        hidden = tokens[step_at]
        for layer_at in range(LAYERS):
            normed = rms_normed(hidden, norm_gain[layer_at])
            combined = routed_sum(normed, expert_ids[layer_at, step_at], gate_weights[layer_at, step_at], is_live, expert_gate_up[layer_at], expert_down[layer_at])
            shared = swiglu(normed, shared_gate_up[layer_at], shared_down[layer_at], SHARED)
            combined = combined + shared.astype(jnp.float32)
            hidden = (hidden.astype(jnp.float32) + jnp.where(is_live[:, None], combined, 0.0)).astype(jnp.bfloat16)
        results.append(hidden)
    return jnp.stack(results)
```

```python
import functools

import jax
import jax.numpy as jnp
from jax import lax
from jax.experimental import pallas as pl
from jax.experimental.pallas import tpu as pltpu
from jax.sharding import PartitionSpec as P

EXPERTS = 16
EPSILON = 1e-06
LANES = 128
BF16 = jnp.bfloat16
F32 = jnp.float32


def dotted(left, right):
    return jnp.dot(left, right, preferred_element_type=F32)


def dotted_nt(left, right):
    return lax.dot_general(left, right, (((1,), (1,)), ((), ())), preferred_element_type=F32)


def layer_kernel(
    n,
    experts,
    group,
    chunk,
    window,
    x_chunk,
    tokens_ref,
    live_ref,
    ids_ref,
    gates_ref,
    gain_ref,
    gate_up_hbm,
    down_hbm,
    shared_up_hbm,
    shared_down_hbm,
    out_ref,
    acc,
    own_n,
    peer_n,
    x_all,
    x_win,
    gate_up,
    down,
    shared_up,
    shared_down,
    up_acc,
    hidden,
    sh_part,
    sh_send,
    sh_peer,
    sh_y,
    sh_yr,
    sh_z,
    sh_zr,
    sh_hidden,
    so_send,
    so_recv,
    so_f,
    so_fr,
    r_p,
    r_pr,
    r_y,
    r_yr,
    r_z,
    r_zr,
    keep,
    res,
    res_r,
    w_sem,
    n_sem,
    win_s,
    win_r,
    xz_s,
    xy_s,
    xp_s,
    x_r,
    hz_s,
    hy_s,
    hp_s,
    h_r,
    sp_sem,
    sy_sem,
    sz_s,
    sz_r,
    so_s,
    so_r,
    p_s,
    p_r,
    y_s,
    y_r,
    z_s,
    z_r,
    f_sem,
    l_sem,
):
    nc = n // 2
    na = nc // 2
    me = lax.axis_index("expert")
    c = lax.rem(me, 2)
    chip = lax.div(me, 2)
    b = lax.rem(chip, 2)
    a = lax.div(chip, 2)
    slot = b * na + a
    oc = 1 - c
    steps, rows_dev, width = tokens_ref.shape
    half = width // 2
    rows = steps * rows_dev
    pair = 2 * rows
    total_rows = nc * pair
    y_rows = na * pair
    units = down.shape[0]
    s_units = sh_part.shape[2]
    fb = shared_down.shape[0]
    x_count = half // x_chunk
    chunks = half // chunk

    def dev(a_at, b_at, c_at):
        return {"expert": (2 * a_at + b_at) * 2 + c_at}

    partner = dev(a, b, oc)
    across = dev(a, 1 - b, c)
    below = dev(a - 1, b, c)
    above = dev(a + 1, b, c)

    def rcopy(src, dst, send, recv, to):
        return pltpu.make_async_remote_copy(
            src_ref=src,
            dst_ref=dst,
            send_sem=send,
            recv_sem=recv,
            device_id=to,
            device_id_type=pl.DeviceIdType.MESH,
        )

    def a_of(d):
        return lax.rem(a + d, na)

    def a_from(d):
        return lax.rem(a + na - d, na)

    def block(at):
        return pl.ds(pl.multiple_of(at * pair, pair), pair)

    loads = []
    offset = lax.rem(me, nc) * fb
    start = lax.div(offset, LANES) * LANES
    inner = pl.multiple_of(offset - start, 16)
    loads.append(
        pltpu.make_async_copy(
            shared_up_hbm.at[0], shared_up.at[pl.ds(inner, fb)], w_sem.at[0]
        )
    )
    for at in range(x_count):
        for side in range(2):
            piece = pl.ds(side * half + at * x_chunk, x_chunk)
            loads.append(
                pltpu.make_async_copy(
                    gate_up_hbm.at[0, 0, piece],
                    gate_up.at[piece],
                    w_sem.at[1 + 2 * at + side],
                )
            )
    down_first = len(loads)
    down_rows = units // 4
    for at in range(4):
        piece = pl.ds(at * down_rows, down_rows)
        loads.append(
            pltpu.make_async_copy(
                down_hbm.at[0, 0, piece], down.at[piece], w_sem.at[down_first + at]
            )
        )
    shared_down_at = len(loads)
    loads.append(
        pltpu.make_async_copy(shared_down_hbm.at[0], shared_down, w_sem.at[shared_down_at])
    )
    shared_up[...] = jnp.zeros_like(shared_up)

    barrier = pltpu.get_barrier_semaphore()
    for d in range(1, n):
        pl.semaphore_signal(
            barrier,
            inc=1,
            device_id={"expert": lax.rem(me + d, n)},
            device_id_type=pl.DeviceIdType.MESH,
        )
    for load in loads:
        load.start()

    lane = lax.broadcasted_iota(jnp.int32, (rows_dev, LANES), 1)
    row_at = lax.broadcasted_iota(jnp.int32, (rows_dev, LANES), 0)
    of_lane = lane & (experts - 1)
    level = lax.div(lane, experts)
    gain = gain_ref[...]
    for step in range(steps):
        h = tokens_ref[step].astype(F32)
        scaling = lax.rsqrt(jnp.mean(h * h, axis=-1, keepdims=True) + EPSILON)
        normed = (h * scaling * gain).astype(BF16).astype(F32)
        ids = ids_ref[0, step]
        gates = gates_ref[0, step]
        dense = jnp.zeros((rows_dev, LANES), F32)
        for k in range(ids.shape[1]):
            dense = dense + jnp.where(ids[:, k : k + 1] == of_lane, gates[:, k : k + 1], 0.0)
        dense = jnp.where(row_at < live_ref[:, step : step + 1], dense, 0.0)
        high = dense.astype(BF16).astype(F32)
        rest = dense - high
        mid = rest.astype(BF16).astype(F32)
        low = rest - mid
        coded = jnp.where(
            level == 0, high, jnp.where(level == 1, mid, jnp.where(level == 2, low, 0.0))
        )
        at = slice(step * rows_dev, (step + 1) * rows_dev)
        for side in range(2):
            own_n[side, at, :half] = normed[:, side * half : (side + 1) * half]
            own_n[side, at, half:] = coded

    pl.semaphore_wait(barrier, n - 1)

    swap = rcopy(own_n.at[oc], peer_n, n_sem.at[0], n_sem.at[1], partner)
    swap.start()
    swap.wait()
    mine = own_n[c]
    theirs = peer_n[...]
    first = jnp.where(c == 0, mine, theirs)
    second = jnp.where(c == 0, theirs, mine)
    x_all[c, block(slot)] = jnp.concatenate([first, second], axis=0).astype(BF16)

    def window_copy(i):
        lo = i * fb // LANES * LANES
        source = x_all.at[c, block(slot), pl.ds(lo, window)]
        return source, x_win.at[slot], win_r.at[slot], c * nc + i

    for i in range(nc):
        source, target, recv, to = window_copy(i)

        @pl.when(to != me)
        def _():
            rcopy(source, target, win_s.at[i], recv, {"expert": to}).start()

        @pl.when(to == me)
        def _():
            pltpu.make_async_copy(source, target, recv).start()

    def x_view(side, at, k):
        wide = x_chunk + (LANES if k == x_count - 1 else 0)
        return x_all.at[side, block(at), pl.ds(k * x_chunk, wide)]

    def x_push(at, k, send, to):
        view = x_view(c, at, k)
        rcopy(view, view, send, x_r.at[c, at, k], to).start()

    def x_arrived(side, at, k):
        view = x_view(side, at, k)
        rcopy(view, view, xp_s.at[0], x_r.at[side, at, k], partner).wait_recv()

    def x_pass(source, k, down_line, up_line):
        at = b * na + source

        @pl.when(down_line & (a > 0))
        def _():
            x_push(at, k, xz_s.at[0, source], below)

        @pl.when(up_line & (a < na - 1))
        def _():
            x_push(at, k, xz_s.at[1, source], above)

        x_push(at, k, xy_s.at[source], across)
        x_push(at, k, xp_s.at[at], partner)

    def at_distance(d, body):
        if d == 0:
            body(a, True, True)
            return

        @pl.when(a + d < na)
        def _():
            body(a + d, True, False)

        @pl.when(a - d >= 0)
        def _():
            body(a - d, False, True)

    def x_along(d):
        for k in range(x_count):

            def one(source, down_line, up_line):
                if d:
                    x_arrived(c, b * na + source, k)
                x_pass(source, k, down_line, up_line)

            at_distance(d, one)

    def x_crossed(d, k):
        def one(source, down_line, up_line):
            at = (1 - b) * na + source
            x_arrived(c, at, k)
            x_push(at, k, xp_s.at[at], partner)

        at_distance(d, one)

    def x_sent(source, down_line, up_line):
        at = b * na + source
        view = x_all.at[c, block(at)]
        other = (1 - b) * na + source

        @pl.when(down_line & (a > 0))
        def _():
            rcopy(view, view, xz_s.at[0, source], x_r.at[c, 0, 0], partner).wait_send()

        @pl.when(up_line & (a < na - 1))
        def _():
            rcopy(view, view, xz_s.at[1, source], x_r.at[c, 0, 0], partner).wait_send()

        rcopy(view, view, xy_s.at[source], x_r.at[c, 0, 0], partner).wait_send()
        rcopy(view, view, xp_s.at[at], x_r.at[c, 0, 0], partner).wait_send()
        rcopy(view, view, xp_s.at[other], x_r.at[c, 0, 0], partner).wait_send()

    def gather(buf, zs, ys, ps, rs):
        sent = []

        def push(at, send, to):
            copy = rcopy(buf.at[c, block(at)], buf.at[c, block(at)], send, rs.at[c, at], to)
            copy.start()
            sent.append(copy)

        def arrived(side, at):
            view = buf.at[side, block(at)]
            rcopy(view, view, ps.at[0], rs.at[side, at], partner).wait_recv()

        def begin():
            for d in range(1, na):
                push(slot, zs.at[d], dev(a_of(d), b, c))
            push(slot, ys.at[0], across)
            push(slot, ps.at[0], partner)

        def forward():
            for d in range(1, na):
                at = b * na + a_from(d)
                arrived(c, at)
                push(at, ys.at[d], across)
                push(at, ps.at[d], partner)

        def finish():
            for d in range(na):
                at = (1 - b) * na + a_from(d)
                arrived(c, at)
                push(at, ps.at[na + d], partner)
            for at in range(nc):
                arrived(oc, at)

        return begin, forward, finish, sent

    s_half = s_units // 2

    def shared_project():
        loads[0].wait()
        for at in range(nc):
            view = x_win.at[at]
            rcopy(view, view, win_s.at[0], win_r.at[at], partner).wait_recv()
        features = x_win[...].reshape(total_rows, window)
        for side in range(2):
            for kind in range(2):
                cols = slice(kind * s_units + side * s_half, kind * s_units + (side + 1) * s_half)
                sh_part[side, :, kind * s_half : (kind + 1) * s_half] = dotted(
                    features, shared_up[:, cols]
                )
        sh_send[...] = sh_part[oc].astype(BF16)
        copy = rcopy(sh_send, sh_peer, sp_sem.at[0], sp_sem.at[1], partner)
        copy.start()
        return copy

    y_own = pl.ds(pl.multiple_of(b * y_rows, y_rows), y_rows)
    y_other = pl.ds(pl.multiple_of((1 - b) * y_rows, y_rows), y_rows)

    def shared_across(copy):
        copy.wait()
        sh_y[...] = (sh_part[c, y_other] + sh_peer[y_other].astype(F32)).astype(BF16)
        out = rcopy(sh_y, sh_yr, sy_sem.at[0], sy_sem.at[1], across)
        out.start()
        return out

    def shared_along(copy):
        copy.wait()
        summed = sh_part[c, y_own] + sh_peer[y_own].astype(F32) + sh_yr[...].astype(F32)
        sh_part[0, :y_rows] = summed
        sh_z[...] = summed.astype(BF16).reshape(na, pair, s_units)
        copies = []
        for d in range(1, na):
            copy = rcopy(
                sh_z.at[a_of(d)],
                sh_zr.at[d],
                sz_s.at[d],
                sz_r.at[d],
                dev(a_of(d), b, c),
            )
            copy.start()
            copies.append(copy)
        return copies

    h_begin, h_forward, h_finish, h_sent = gather(sh_hidden, hz_s, hy_s, hp_s, h_r)

    def shared_active(copies):
        total = sh_part[0, block(a)]
        for d in range(1, na):
            copies[d - 1].wait()
            total = total + sh_zr[d].astype(F32)
        sh_hidden[c, block(slot)] = (
            jax.nn.silu(total[:, :s_half]) * total[:, s_half:]
        ).astype(BF16)
        h_begin()

    def shared_last():
        h_finish()
        loads[shared_down_at].wait()
        cols = dotted_nt(sh_hidden[0], shared_down[:, :s_half]) + dotted_nt(
            sh_hidden[1], shared_down[:, s_half:]
        )
        so_send[...] = cols.astype(BF16).reshape(nc, pair, fb)
        copies = []
        for d in range(1, nc):
            other = lax.rem(chip + d, nc)
            to_slot = lax.rem(other, 2) * na + lax.div(other, 2)
            copy = rcopy(
                so_send.at[to_slot],
                so_recv.at[chip],
                so_s.at[d],
                so_r.at[chip],
                {"expert": other * 2 + c},
            )
            copy.start()
            copies.append(copy)
        return copies

    def shared_collect(copies):
        for d in range(1, nc):
            other = lax.rem(chip + nc - d, nc)
            view = so_recv.at[other]
            rcopy(view, view, so_s.at[0], so_r.at[other], partner).wait_recv()
        so_recv[chip] = so_send[slot]
        for at in range(nc):
            value = so_recv[at].astype(F32)
            so_f[0, at] = value[:rows]
            so_f[1, at] = value[rows:]
        copy = rcopy(so_f.at[oc], so_fr, f_sem.at[0], f_sem.at[1], partner)
        copy.start()
        for copy_at in copies:
            copy_at.wait_send()
        return copy

    def up_term(k, cols):
        at = k * x_chunk
        return dotted(x_all[0, :, at : at + x_chunk], gate_up[at : at + x_chunk, cols]) + dotted(
            x_all[1, :, at : at + x_chunk], gate_up[half + at : half + at + x_chunk, cols]
        )

    tile = min(256, units)

    def up_part(k):
        for at in range(nc):
            x_arrived(oc, at, k)
        for side in range(2):
            loads[1 + 2 * k + side].wait()
        if k < x_count - 1:
            for at in range(2 * units // tile):
                cols = slice(at * tile, (at + 1) * tile)
                if k == 0:
                    up_acc[:, cols] = up_term(k, cols)
                else:
                    up_acc[:, cols] += up_term(k, cols)
            return
        for at in range(units // tile):
            gate_cols = slice(at * tile, (at + 1) * tile)
            up_cols = slice(units + at * tile, units + (at + 1) * tile)
            gate = up_term(k, gate_cols)
            up = up_term(k, up_cols)
            if k:
                gate = gate + up_acc[:, gate_cols]
                up = up + up_acc[:, up_cols]
            hidden[:, gate_cols] = (jax.nn.silu(gate) * up).astype(BF16)

    state = []
    x_along(0)
    for d in range(1, na):
        x_along(d)
        for k in range(x_count):
            x_crossed(d - 1, k)
        if d == 1:
            state.append(shared_project())
        if d == min(2, na - 1):
            state.append(shared_across(state[-1]))
    lag = min(2, x_count - 1)
    for k in range(x_count + lag):
        if k < x_count:
            x_crossed(na - 1, k)
        if k >= lag:
            up_part(k - lag)
            if k - lag == x_count // 2:
                state.append(shared_along(state[-1]))

    expert = lax.div(me, group)
    codes = x_all[0, :, half:].astype(F32)
    wide = lax.broadcasted_iota(jnp.int32, (total_rows, LANES), 1) & (experts - 1)
    weight = jnp.sum(jnp.where(wide == expert, codes, 0.0), axis=1, keepdims=True)

    for load in loads[down_first:shared_down_at]:
        load.wait()

    def product(side, j):
        cols = pl.ds(pl.multiple_of(side * half + j * chunk, LANES), chunk)
        return dotted(hidden[...], down[:, cols]) * weight

    def send_partner(j):
        r_p[j] = product(oc, j).astype(BF16)
        rcopy(r_p.at[j], r_pr.at[j], p_s.at[0], p_r.at[j], partner).start()

    far = jnp.where(2 * a >= na, 0, na - 1)

    def send_across(at, j):
        rcopy(r_y.at[at, j], r_yr.at[at, j], y_s.at[at], y_r.at[at, j], across).start()

    def own_part(j):
        mine = product(c, j)
        rcopy(r_p.at[j], r_pr.at[j], p_s.at[0], p_r.at[j], partner).wait_recv()
        up_acc[:, :chunk] = mine
        other = (up_acc[y_other, :chunk] + r_pr[j, y_other].astype(F32)).astype(BF16)
        for at in range(na):
            r_y[at, j] = other[at * pair : (at + 1) * pair]
        send_across(far, j)
        here = up_acc[y_own, :chunk] + r_pr[j, y_own].astype(F32)
        for at in range(na):
            keep[at, j] = here[at * pair : (at + 1) * pair]

    def y_arrived(at, j):
        rcopy(r_y.at[at, j], r_yr.at[at, j], y_s.at[at], y_r.at[at, j], across).wait_recv()

    def z_arrived(way, at, j):
        view = r_zr.at[way, at, j]
        rcopy(view, view, z_s.at[at], z_r.at[way, at, j], across).wait_recv()

    def z_pass(d, j):
        def one(at, up_line, down_line):
            way, inside, to = (1, a > 0, above) if up_line else (0, a < na - 1, below)
            y_arrived(at, j)
            summed = keep[at, j] + r_yr[at, j].astype(F32)

            @pl.when(inside)
            def _():
                z_arrived(way, at, j)
                r_z[at, j] = (summed + r_zr[way, at, j].astype(F32)).astype(BF16)

            @pl.when(jnp.logical_not(inside))
            def _():
                r_z[at, j] = summed.astype(BF16)

            rcopy(r_z.at[at, j], r_zr.at[way, at, j], z_s.at[at], z_r.at[way, at, j], to).start()

        at_distance(d, one)

    def collect(j):
        y_arrived(a, j)
        keep[a, j] = keep[a, j] + r_yr[a, j].astype(F32)
        for way, inside in ((1, a > 0), (0, a < na - 1)):

            @pl.when(inside)
            def _():
                z_arrived(way, a, j)
                keep[a, j] = keep[a, j] + r_zr[way, a, j].astype(F32)

        total = keep[a, j]
        res[0, j] = total[:rows]
        res[1, j] = total[rows:]
        rcopy(res.at[oc, j], res_r.at[j], l_sem.at[0, j], l_sem.at[1, j], partner).start()

    lead = min(2, chunks)
    for j in range(lead):
        send_partner(j)
    for j in range(chunks):
        if j + lead < chunks:
            send_partner(j + lead)
        own_part(j)
    for d in range(na - 1, -1, -1):

        def rest(at, up_line, down_line):
            @pl.when(at != far)
            def _():
                for j in range(chunks):
                    send_across(at, j)

        at_distance(d, rest)
    shared_active(state[-1])
    for d in range(na - 1, 0, -1):
        for j in range(chunks):
            z_pass(d, j)
        if d == na - 1:
            h_forward()
        if d == max(1, na - 2):
            state.append(shared_last())
    shared_swap = shared_collect(state[-1])
    for j in range(chunks):
        collect(j)
    for j in range(chunks):
        rcopy(res.at[oc, j], res_r.at[j], l_sem.at[0, j], l_sem.at[1, j], partner).wait()
        own_cols = pl.ds(pl.multiple_of(c * half + j * chunk, LANES), chunk)
        other_cols = pl.ds(pl.multiple_of(oc * half + j * chunk, LANES), chunk)
        acc[:, own_cols] = res[c, j]
        acc[:, other_cols] = res_r[j]
    shared_swap.wait()
    for at in range(nc):
        slot_chip = so_f[c, at]
        peer_chip = so_fr[at]
        for side in range(2):
            cols = slice((2 * at + side) * fb, (2 * at + side + 1) * fb)
            acc[:, cols] = acc[:, cols] + jnp.where(c == side, slot_chip, peer_chip)
    row_of = lax.broadcasted_iota(jnp.int32, (rows_dev, width), 0)
    for step in range(steps):
        update = acc[step * rows_dev : (step + 1) * rows_dev]
        update = jnp.where(row_of < live_ref[:, step : step + 1], update, 0.0)
        out_ref[step] = (tokens_ref[step].astype(F32) + update).astype(BF16)
    for i in range(nc):
        source, target, recv, to = window_copy(i)

        @pl.when(to != me)
        def _():
            rcopy(source, target, win_s.at[i], recv, {"expert": to}).wait_send()

    for d in range(na):
        at_distance(d, x_sent)
    for copy in h_sent:
        copy.wait_send()
    rcopy(r_p, r_pr, p_s.at[0], p_r.at[0], partner).wait_send()
    for at in range(na):
        rcopy(r_y.at[at], r_yr.at[at], y_s.at[at], y_r.at[at, 0], across).wait_send()

        @pl.when(a != at)
        def _():
            rcopy(r_z.at[at], r_zr.at[0, at], z_s.at[at], z_r.at[0, at, 0], across).wait_send()


def per_device(
    tokens,
    live_rows,
    expert_ids,
    gate_weights,
    norm_gain,
    expert_gate_up,
    expert_down,
    shared_gate_up,
    shared_down,
):
    step_count, row_count, model_width = tokens.shape
    n = lax.axis_size("expert")
    group = n // EXPERTS
    units = expert_down.shape[2]
    fb, s_wide = shared_gate_up.shape[1:]
    s_units = s_wide // 2
    nc = n // 2
    na = nc // 2
    half = model_width // 2
    rows = step_count * row_count
    pair = 2 * rows
    total = nc * pair
    y_rows = na * pair
    wide = half + LANES
    chunk = next(size for size in (512, 256, 128) if half % size == 0)
    chunks = half // chunk
    span = next(size for size in (128, 64, 32, 16) if fb % size == 0)
    window = -(-(fb + LANES - span) // LANES) * LANES
    dma = pltpu.SemaphoreType.DMA
    vmem = pltpu.VMEM
    whole = pl.BlockSpec(memory_space=pltpu.VMEM)
    anywhere = pl.BlockSpec(memory_space=pl.ANY)
    x_chunk = chunk if nc <= EXPERTS else half
    x_count = half // x_chunk
    return pl.pallas_call(
        functools.partial(layer_kernel, n, EXPERTS, group, chunk, window, x_chunk),
        out_shape=jax.ShapeDtypeStruct(tokens.shape, BF16),
        in_specs=[whole] * 5 + [anywhere] * 4,
        out_specs=whole,
        scratch_shapes=[
            vmem((rows, model_width), F32),
            vmem((2, rows, wide), F32),
            vmem((rows, wide), F32),
            vmem((2, total, wide), BF16),
            vmem((nc, pair, window), BF16),
            vmem((model_width, 2 * units), BF16),
            vmem((units, model_width), BF16),
            vmem((window, s_wide), BF16),
            vmem((fb, s_units), BF16),
            vmem((total, max(2 * units, chunk)), F32),
            vmem((total, units), BF16),
            vmem((2, total, s_units), F32),
            vmem((total, s_units), BF16),
            vmem((total, s_units), BF16),
            vmem((y_rows, s_units), BF16),
            vmem((y_rows, s_units), BF16),
            vmem((na, pair, s_units), BF16),
            vmem((na, pair, s_units), BF16),
            vmem((2, total, s_units // 2), BF16),
            vmem((nc, pair, fb), BF16),
            vmem((nc, pair, fb), BF16),
            vmem((2, nc, rows, fb), F32),
            vmem((nc, rows, fb), F32),
            vmem((chunks, total, chunk), BF16),
            vmem((chunks, total, chunk), BF16),
            vmem((na, chunks, pair, chunk), BF16),
            vmem((na, chunks, pair, chunk), BF16),
            vmem((na, chunks, pair, chunk), BF16),
            vmem((2, na, chunks, pair, chunk), BF16),
            vmem((na, chunks, pair, chunk), F32),
            vmem((2, chunks, rows, chunk), F32),
            vmem((chunks, rows, chunk), F32),
            dma((2 * x_count + 6,)),
            dma((2,)),
            dma((nc,)),
            dma((nc,)),
            dma((2, na)),
            dma((na,)),
            dma((nc,)),
            dma((2, nc, x_count)),
            dma((na,)),
            dma((na,)),
            dma((nc,)),
            dma((2, nc)),
            dma((2,)),
            dma((2,)),
            dma((na,)),
            dma((na,)),
            dma((nc,)),
            dma((nc,)),
            dma((1,)),
            dma((chunks,)),
            dma((na,)),
            dma((na, chunks)),
            dma((na,)),
            dma((2, na, chunks)),
            dma((2,)),
            dma((2, chunks)),
        ],
        compiler_params=pltpu.CompilerParams(
            collective_id=0, has_side_effects=True, vmem_limit_bytes=67_043_328
        ),
    )(
        tokens,
        live_rows.T,
        expert_ids,
        gate_weights,
        norm_gain,
        expert_gate_up,
        expert_down,
        shared_gate_up,
        jnp.swapaxes(shared_down, 1, 2),
    )


def solution(mesh):
    placed = (
        P(None, ("parts", "expert"), None),
        P(None, ("parts", "expert")),
        P(None, None, ("parts", "expert"), None),
        P(None, None, ("parts", "expert"), None),
        P(),
        P(None, "expert", None, None),
        P(None, "expert", None, None),
        P(None, "expert", None),
        P(None, None, "expert"),
    )
    return jax.shard_map(
        per_device,
        mesh=mesh,
        in_specs=placed,
        out_specs=P(None, ("parts", "expert"), None),
        check_vma=False,
    )
```

```python
import functools

import jax
import jax.numpy as jnp
from jax import lax
from jax.experimental import pallas as pl
from jax.experimental.pallas import tpu as pltpu
from jax.sharding import PartitionSpec as P

EXPERTS = 16
EPSILON = 1e-06
LANES = 128
X_TURNED = 3
R_TURNED = 2
GROUPED = 2
AT_PROJECT = 4
AT_ACROSS = 10
BF16 = jnp.bfloat16
F32 = jnp.float32


def dotted(left, right):
    return jnp.dot(left, right, preferred_element_type=F32)


def dotted_nt(left, right):
    return lax.dot_general(left, right, (((1,), (1,)), ((), ())), preferred_element_type=F32)


def layer_kernel(
    n,
    experts,
    group,
    chunk,
    window,
    x_chunk,
    x_turned,
    r_turned,
    tokens_ref,
    live_ref,
    ids_ref,
    gates_ref,
    gain_ref,
    gate_up_hbm,
    down_hbm,
    shared_up_hbm,
    shared_down_hbm,
    out_ref,
    acc,
    own_n,
    peer_n,
    x_all,
    x_win,
    gate_up,
    down,
    shared_up,
    shared_down,
    up_acc,
    hidden,
    sh_part,
    sh_send,
    sh_peer,
    sh_z,
    sh_zr,
    sh_hidden,
    so_send,
    so_recv,
    r_p,
    r_pr,
    r_y,
    r_yr,
    r_z,
    r_zr,
    r_cr,
    cross,
    keep,
    res,
    res_r,
    w_sem,
    n_sem,
    win_s,
    win_r,
    xz_s,
    xc_s,
    xy_s,
    xp_s,
    x_r,
    xp_r,
    h_sem,
    sp_sem,
    sz_sem,
    so_sem,
    p_s,
    p_r,
    c_s,
    c_r,
    y_s,
    y_r,
    z_s,
    z_r,
    l_s,
    l_r,
):
    nc = n // 2
    na = nc // 2
    me = lax.axis_index("expert")
    barrier = pltpu.get_barrier_semaphore()
    for d in range(1, n):
        pl.semaphore_signal(
            barrier,
            inc=1,
            device_id={"expert": lax.rem(me + d, n)},
            device_id_type=pl.DeviceIdType.MESH,
        )
    c = lax.rem(me, 2)
    chip = lax.div(me, 2)
    b = lax.rem(chip, 2)
    a = lax.div(chip, 2)
    slot = b * na + a
    oc = 1 - c
    steps, rows_dev, width = tokens_ref.shape
    half = width // 2
    rows = steps * rows_dev
    pair = 2 * rows
    total_rows = nc * pair
    y_rows = na * pair
    units = down.shape[0]
    s_units = sh_part.shape[2]
    fb = shared_down.shape[0]
    x_count = half // x_chunk
    chunks = half // chunk

    def dev(a_at, b_at, c_at):
        return {"expert": (2 * a_at + b_at) * 2 + c_at}

    partner = dev(a, b, oc)
    across = dev(a, 1 - b, c)
    below = dev(a - 1, b, c)
    above = dev(a + 1, b, c)

    def rcopy(src, dst, send, recv, to):
        return pltpu.make_async_remote_copy(
            src_ref=src,
            dst_ref=dst,
            send_sem=send,
            recv_sem=recv,
            device_id=to,
            device_id_type=pl.DeviceIdType.MESH,
        )

    def a_of(d):
        return lax.rem(a + d, na)

    def block(at):
        return pl.ds(pl.multiple_of(at * pair, pair), pair)

    loads = []
    offset = lax.rem(me, nc) * fb
    start = lax.div(offset, LANES) * LANES
    inner = pl.multiple_of(offset - start, 16)
    loads.append(
        pltpu.make_async_copy(
            shared_up_hbm.at[0], shared_up.at[pl.ds(inner, fb)], w_sem.at[0]
        )
    )
    for at in range(x_count):
        for side in range(2):
            piece = pl.ds(side * half + at * x_chunk, x_chunk)
            loads.append(
                pltpu.make_async_copy(
                    gate_up_hbm.at[0, 0, piece], gate_up.at[piece], w_sem.at[3 + at]
                )
            )
    loads.append(pltpu.make_async_copy(down_hbm.at[0, 0], down, w_sem.at[1]))
    down_load = loads[-1]
    loads.append(pltpu.make_async_copy(shared_down_hbm.at[0], shared_down, w_sem.at[2]))
    shared_down_load = loads[-1]

    def gate_up_wait(k):
        view = gate_up.at[pl.ds(0, 2 * x_chunk)]
        pltpu.make_async_copy(view, view, w_sem.at[3 + k]).wait()

    shared_up[...] = jnp.zeros_like(shared_up)

    for load in loads:
        load.start()

    lane = lax.broadcasted_iota(jnp.int32, (rows_dev, LANES), 1)
    row_at = lax.broadcasted_iota(jnp.int32, (rows_dev, LANES), 0)
    of_lane = lane & (experts - 1)
    level = lax.div(lane, experts)
    gain = gain_ref[...]
    for step in range(steps):
        h = tokens_ref[step].astype(F32)
        scaling = lax.rsqrt(jnp.mean(h * h, axis=-1, keepdims=True) + EPSILON)
        normed = (h * scaling * gain).astype(BF16).astype(F32)
        ids = ids_ref[0, step]
        gates = gates_ref[0, step]
        dense = jnp.zeros((rows_dev, LANES), F32)
        for k in range(ids.shape[1]):
            dense = dense + jnp.where(ids[:, k : k + 1] == of_lane, gates[:, k : k + 1], 0.0)
        dense = jnp.where(row_at < live_ref[:, step : step + 1], dense, 0.0)
        high = dense.astype(BF16).astype(F32)
        rest = dense - high
        mid = rest.astype(BF16).astype(F32)
        low = rest - mid
        coded = jnp.where(
            level == 0, high, jnp.where(level == 1, mid, jnp.where(level == 2, low, 0.0))
        )
        at = slice(step * rows_dev, (step + 1) * rows_dev)
        for side in range(2):
            own_n[side, at, :half] = normed[:, side * half : (side + 1) * half]
            own_n[side, at, half:] = coded

    pl.semaphore_wait(barrier, n - 1)

    swap = rcopy(own_n.at[oc], peer_n, n_sem.at[0], n_sem.at[1], partner)
    swap.start()
    swap.wait()
    mine = own_n[c]
    theirs = peer_n[...]
    first = jnp.where(c == 0, mine, theirs)
    second = jnp.where(c == 0, theirs, mine)
    x_all[c, block(slot)] = jnp.concatenate([first, second], axis=0).astype(BF16)

    def window_copy(i):
        lo = i * fb // LANES * LANES
        source = x_all.at[c, block(slot), pl.ds(lo, window)]
        return source, x_win.at[slot], win_r.at[0], c * nc + i

    def x_view(side, at, k):
        wide = x_chunk + (LANES if k == x_count - 1 else 0)
        return x_all.at[side, block(at), pl.ds(k * x_chunk, wide)]

    def x_push(at, k, send, to):
        view = x_view(c, at, k)
        rcopy(view, view, send, x_r.at[at, k], to).start()

    def x_twin(at, k):
        view = x_view(c, at, k)
        rcopy(view, view, xp_s.at[0], xp_r.at[k], partner).start()

    def x_arrived(at, k):
        view = x_view(c, at, k)
        rcopy(view, view, xp_s.at[0], x_r.at[at, k], partner).wait_recv()

    gate_down = lax.rem(a, 2) == 1
    gate_up_way = lax.rem(na - 1 - a, 2) == 1

    def x_steps(d, down_line, up_line):
        for way, line, gate in ((0, down_line, gate_down), (1, up_line, gate_up_way)):
            for step in (1, 2):
                if line:
                    inside = a >= step if way == 0 else a < na - step
                    goes = inside if d == 0 and step == 1 else inside & gate
                    yield way, step, goes, dev(a - step if way == 0 else a + step, b, c)

    def at_distance(d, body):
        if d == 0:
            body(a, True, True)
            return

        @pl.when(a + d < na)
        def _():
            body(a + d, True, False)

        @pl.when(a - d >= 0)
        def _():
            body(a - d, False, True)

    def x_along(d, k, gates=True):
        if not 0 <= k < x_count:
            return

        def one(source, down_line, up_line):
            at = b * na + source

            def handle():
                if d:
                    x_arrived(at, k)
                for way, step, goes, to in x_steps(d, down_line, up_line):

                    @pl.when(goes)
                    def _():
                        x_push(at, k, xz_s.at[way, step - 1, source], to)

                if d != 1 or k >= x_turned:
                    x_push(at, k, xy_s.at[source], across)
                x_twin(at, k)

            if d < 2:
                handle()
            else:
                gate = gate_down if down_line else gate_up_way
                pl.when(gate if gates else jnp.logical_not(gate))(handle)

        at_distance(d, one)

    def x_crossed(d, k):
        if not 0 <= k < x_count:
            return

        def one(source, down_line, up_line):
            at = (1 - b) * na + source
            x_arrived(at, k)
            if d == 0 and k < x_turned:
                for way, inside, to in ((0, a > 0, below), (1, a < na - 1, above)):

                    @pl.when(inside)
                    def _():
                        x_push(at, k, xc_s.at[way], to)

            x_twin(at, k)

        at_distance(d, one)

    def x_sent(d):
        def sent(sem, lo=0, hi=half + LANES):
            if lo < hi:
                view = x_all.at[c, block(0), pl.ds(lo, hi - lo)]
                rcopy(view, view, sem, x_r.at[0, 0], partner).wait_send()

        turned = half + LANES if x_turned == x_count else x_turned * x_chunk

        def one(source, down_line, up_line):
            for way, step, goes, _ in x_steps(d, down_line, up_line):

                @pl.when(goes)
                def _():
                    sent(xz_s.at[way, step - 1, source])

            if d == 0:
                for way, inside in ((0, a > 0), (1, a < na - 1)):

                    @pl.when(inside)
                    def _():
                        sent(xc_s.at[way], 0, turned)

            sent(xy_s.at[source], turned if d == 1 else 0)

        at_distance(d, one)

    s_half = s_units // 2

    def shared_project():
        loads[0].wait()
        rcopy(x_win, x_win, win_s.at[0], win_r.at[0], partner).wait_recv()
        features = x_win[...].reshape(total_rows, window)
        for side in range(2):
            for kind in range(2):
                cols = slice(kind * s_units + side * s_half, kind * s_units + (side + 1) * s_half)
                sh_part[side, :, kind * s_half : (kind + 1) * s_half] = dotted(
                    features, shared_up[:, cols]
                )
        sh_send[...] = sh_part[oc].astype(BF16)
        copy = rcopy(sh_send, sh_peer, sp_sem.at[0], sp_sem.at[1], partner)
        copy.start()
        return copy

    y_own = pl.ds(pl.multiple_of(b * y_rows, y_rows), y_rows)
    y_other = pl.ds(pl.multiple_of((1 - b) * y_rows, y_rows), y_rows)

    def shared_spread(copy):
        copy.wait()
        sh_part[0] = sh_part[c] + sh_peer[...].astype(F32)
        sh_z[...] = sh_part[0].astype(BF16).reshape(nc, pair, s_units)
        for d in range(1, nc):
            other = lax.rem(chip + d, nc)
            rcopy(
                sh_z.at[lax.rem(other, 2) * na + lax.div(other, 2)],
                sh_zr.at[d - 1],
                sz_sem.at[0],
                sz_sem.at[1],
                {"expert": other * 2 + c},
            ).start()

    others = pl.ds(0, (nc - 1) * pair)

    def shared_active():
        rcopy(sh_zr, sh_zr, sz_sem.at[0], sz_sem.at[1], partner).wait()
        total = sh_part[0, block(slot)]
        for d in range(1, nc):
            total = total + sh_zr[d - 1].astype(F32)
        sh_hidden[c, block(slot)] = (
            jax.nn.silu(total[:, :s_half]) * total[:, s_half:]
        ).astype(BF16)
        view = sh_hidden.at[c, block(slot)]
        for d in range(1, nc):
            to = {"expert": lax.rem(chip + d, nc) * 2 + c}
            rcopy(view, view, h_sem.at[0], h_sem.at[1], to).start()

    def shared_twin():
        view = sh_hidden.at[c, others]
        rcopy(view, view, h_sem.at[0], h_sem.at[1], partner).wait()
        view = sh_hidden.at[c]
        rcopy(view, view, h_sem.at[2], h_sem.at[3], partner).start()

    def shared_last():
        view = sh_hidden.at[c]
        rcopy(view, view, h_sem.at[2], h_sem.at[3], partner).wait()
        shared_down_load.wait()
        cols = dotted_nt(sh_hidden[0], shared_down[:, :s_half]) + dotted_nt(
            sh_hidden[1], shared_down[:, s_half:]
        )
        cols = cols.reshape(n, rows, fb).astype(BF16)
        for at in range(n):
            owner = 4 * (at // 2 % na) + 2 * (at // 2 // na) + at % 2
            so_send[lax.rem(owner - me + n, n)] = cols[at]
        for d in range(1, n):
            to = {"expert": lax.rem(me + d, n)}
            rcopy(so_send.at[d], so_recv.at[n - d], so_sem.at[0], so_sem.at[1], to).start()
        so_recv[0] = so_send[0]

    def shared_collect():
        view = so_recv.at[pl.ds(1, n - 1)]
        rcopy(view, view, so_sem.at[0], so_sem.at[1], partner).wait()

    def up_term(k, cols):
        at = k * x_chunk
        return dotted(x_all[0, :, at : at + x_chunk], gate_up[at : at + x_chunk, cols]) + dotted(
            x_all[1, :, at : at + x_chunk], gate_up[half + at : half + at + x_chunk, cols]
        )

    tile = min(256, units)

    def up_part(k):
        wide = x_chunk + (LANES if k == x_count - 1 else 0)
        view = x_all.at[oc, :, pl.ds(k * x_chunk, wide)]
        rcopy(view, view, xp_s.at[0], xp_r.at[k], partner).wait_recv()
        gate_up_wait(k)
        if k < x_count - 1:
            for at in range(2 * units // tile):
                cols = slice(at * tile, (at + 1) * tile)
                if k == 0:
                    up_acc[:, cols] = up_term(k, cols)
                else:
                    up_acc[:, cols] += up_term(k, cols)
            return
        for at in range(units // tile):
            gate_cols = slice(at * tile, (at + 1) * tile)
            up_cols = slice(units + at * tile, units + (at + 1) * tile)
            gate = up_term(k, gate_cols)
            up = up_term(k, up_cols)
            if k:
                gate = gate + up_acc[:, gate_cols]
                up = up + up_acc[:, up_cols]
            hidden[:, gate_cols] = (jax.nn.silu(gate) * up).astype(BF16)

    for i in range(nc):
        source, target, recv, to = window_copy(i)

        @pl.when(to != me)
        def _():
            rcopy(source, target, win_s.at[0], recv, {"expert": to}).start()

        @pl.when(to == me)
        def _():
            pltpu.make_async_copy(source, target, recv).start()

    for k in range(x_count):
        x_along(0, k)
    def gate_lag(d):
        return 3 * ((d - 1) // 2)

    def leaf_lag(d):
        return 0 if d < 2 else 3 * ((d - 2) // 2) + 3

    last_lag = leaf_lag(na - 1) + 4
    up_lag = last_lag + 2
    count = x_count + up_lag
    shared_copy = None
    for i in range(count):
        for d in range(1, na):
            x_along(d, i - gate_lag(d))
        x_crossed(0, i)
        for d in range(2, na):
            x_along(d, i - leaf_lag(d), False)
        if i == min(AT_PROJECT, count - 4):
            shared_copy = shared_project()
        if i == min(AT_ACROSS, count - 3):
            shared_spread(shared_copy)
        for d in range(1, na - 1):
            x_crossed(d, i - leaf_lag(d) - 4)
        x_crossed(na - 1, i - last_lag)
        if i >= up_lag:
            up_part(i - up_lag)

    expert = lax.div(me, group)
    codes = x_all[0, :, half:].astype(F32)
    wide = lax.broadcasted_iota(jnp.int32, (total_rows, LANES), 1) & (experts - 1)
    weight = jnp.sum(jnp.where(wide == expert, codes, 0.0), axis=1, keepdims=True)

    down_load.wait()

    def product(side, group):
        wide = chunk * len(group)
        cols = pl.ds(pl.multiple_of(side * half + group[0] * chunk, LANES), wide)
        return dotted(hidden[...], down[:, cols]) * weight

    def send_partner(group):
        sums = product(oc, group).astype(BF16)
        for place, j in enumerate(group):
            r_p[j] = sums[:, place * chunk : (place + 1) * chunk]
        for j in group:
            rcopy(r_p.at[j], r_pr.at[j], p_s.at[0], p_r.at[j], partner).start()

    def send_across(at, j):
        rcopy(r_y.at[at, j], r_yr.at[at, j], y_s.at[at], y_r.at[at, j], across).start()

    cross_rows = block((1 - b) * na + a)

    def own_part(group):
        up_acc[:, : chunk * len(group)] = product(c, group)
        for j in group:
            rcopy(r_p.at[j], r_pr.at[j], p_s.at[0], p_r.at[j], partner).wait_recv()
        for place, j in enumerate(group):
            cols = slice(place * chunk, (place + 1) * chunk)
            other = (up_acc[y_other, cols] + r_pr[j, y_other].astype(F32)).astype(BF16)
            for at in range(na):
                r_y[at, j] = other[at * pair : (at + 1) * pair]
        for place, j in enumerate(group):
            for d in range(na - 1, 1, -1):
                at_distance(d, lambda at, up_line, down_line: send_across(at, j))

            def beside(at, up_line, down_line):
                way, to = (1, above) if up_line else (0, below)
                rcopy(r_y.at[at, j], r_cr.at[way, j], c_s.at[way], c_r.at[way, j], to).start()

            if j < r_turned:
                at_distance(1, beside)
        for place, j in enumerate(group):
            cols = slice(place * chunk, (place + 1) * chunk)
            cross[j] = up_acc[cross_rows, cols] + r_pr[j, cross_rows].astype(F32)
            here = up_acc[y_own, cols] + r_pr[j, y_own].astype(F32)
            for at in range(na):
                keep[at, j] = here[at * pair : (at + 1) * pair]

    def join(j):
        for way, inside in ((1, a > 0), (0, a < na - 1)) if j < r_turned else ():

            @pl.when(inside)
            def _():
                view = r_cr.at[way, j]
                rcopy(view, view, c_s.at[0], c_r.at[way, j], across).wait_recv()
                cross[j] = cross[j] + r_cr[way, j].astype(F32)

        r_y[a, j] = cross[j].astype(BF16)
        send_across(a, j)

    def y_arrived(at, j):
        rcopy(r_y.at[at, j], r_yr.at[at, j], y_s.at[at], y_r.at[at, j], across).wait_recv()

    def z_place(step, place):
        if step == 1 or na > 4:
            return (step - 1) * (na + 1) + place
        return na + 1 + (place is na)

    def z_add(step, place, at, j):
        index = z_place(step, place)
        view = r_zr.at[index, j]
        rcopy(view, view, z_s.at[0], z_r.at[index, j], across).wait_recv()
        keep[at, j] = keep[at, j] + r_zr[index, j].astype(F32)

    def gate_even(up_line):
        return lax.rem(na - 1 - a if up_line else a, 2) == 0

    def leaf(up_line):
        return jnp.logical_not(gate_even(up_line))

    def z_pass(d, j, only=None):
        def one(at, up_line, down_line):
            if only is None:
                forward(at, up_line)
            else:
                pl.when(only(up_line))(lambda: forward(at, up_line))

        def forward(at, up_line):
            if d > 1 or j >= r_turned:
                y_arrived(at, j)
                keep[at, j] = keep[at, j] + r_yr[at, j].astype(F32)
            for step in (1, 2):
                if d + step < na:

                    @pl.when(gate_even(up_line) & (a >= step if up_line else a < na - step))
                    def _():
                        z_add(step, at, at, j)

            r_z[at, j] = keep[at, j].astype(BF16)
            last = na if not up_line else at

            def send(hop, place):
                to = dev(a + hop if up_line else a - hop, b, c)
                index = z_place(hop, place)
                rcopy(
                    r_z.at[at, j], r_zr.at[index, j], z_s.at[0], z_r.at[index, j], to
                ).start()

            if d == 1:
                send(1, last)
            else:
                even = gate_even(up_line)
                pl.when(even)(lambda: send(2, last if d == 2 else at))
                pl.when(jnp.logical_not(even))(lambda: send(1, at))

        at_distance(d, one)

    def collect(j):
        y_arrived(a, j)
        keep[a, j] = keep[a, j] + r_yr[a, j].astype(F32)
        for step in (1, 2):
            for place, inside, up_line in ((a, a >= step, True), (na, a < na - step, False)):
                if step == 2:
                    inside = inside & gate_even(up_line)

                @pl.when(inside)
                def _():
                    z_add(step, place, a, j)

        total = keep[a, j]
        res[0, j] = total[:rows]
        res[1, j] = total[rows:]
        rcopy(res.at[oc, j], res_r.at[j], l_s.at[0], l_r.at[j], partner).start()

    groups = [tuple(range(j, min(j + GROUPED, chunks))) for j in range(0, chunks, GROUPED)]
    send_partner(groups[0])
    for at, group in enumerate(groups):
        if at + 1 < len(groups):
            send_partner(groups[at + 1])
        own_part(group)
        for j in group:
            if j < r_turned:
                z_pass(1, j, leaf)
    shared_active()
    for j in range(r_turned, chunks):
        at_distance(1, lambda at, up_line, down_line: send_across(at, j))
    for j in range(chunks):
        join(j)
    for d in range(na - 1, 2, -1):
        for j in range(chunks):
            z_pass(d, j)
    if na > 2:
        for j in range(chunks):
            z_pass(2, j, leaf)
    shared_twin()
    if na > 2:
        for j in range(chunks):
            z_pass(2, j, gate_even)
    shared_last()
    for j in range(chunks):
        z_pass(1, j, gate_even if j < r_turned else None)
    for j in range(chunks):
        collect(j)
    shared_collect()
    for j in range(chunks):
        rcopy(res.at[oc, j], res_r.at[j], l_s.at[0], l_r.at[j], partner).wait_recv()
        own_cols = pl.ds(pl.multiple_of(c * half + j * chunk, LANES), chunk)
        other_cols = pl.ds(pl.multiple_of(oc * half + j * chunk, LANES), chunk)
        acc[:, own_cols] = res[c, j]
        acc[:, other_cols] = res_r[j]
    for at in range(n):
        cols = slice(at * fb, (at + 1) * fb)
        acc[:, cols] = acc[:, cols] + so_recv[lax.rem(at - me + n, n)].astype(F32)
    row_of = lax.broadcasted_iota(jnp.int32, (rows_dev, width), 0)
    for step in range(steps):
        update = acc[step * rows_dev : (step + 1) * rows_dev]
        update = jnp.where(row_of < live_ref[:, step : step + 1], update, 0.0)
        out_ref[step] = (tokens_ref[step].astype(F32) + update).astype(BF16)
    @pl.when(lax.div(me, nc) == c)
    def _():
        view = x_win.at[pl.ds(0, nc - 1)]
        rcopy(view, view, win_s.at[0], win_r.at[0], partner).wait_send()

    @pl.when(lax.div(me, nc) != c)
    def _():
        rcopy(x_win, x_win, win_s.at[0], win_r.at[0], partner).wait_send()

    for d in range(na):
        x_sent(d)
    view = x_all.at[c]
    rcopy(view, view, xp_s.at[0], xp_r.at[0], partner).wait_send()
    rcopy(r_p, r_pr, p_s.at[0], p_r.at[0], partner).wait_send()
    for d in range(na):
        first = r_turned if d == 1 else 0

        def y_sent(at, up_line, down_line):
            view = r_y.at[at, pl.ds(first, chunks - first)]
            rcopy(view, view, y_s.at[at], y_r.at[0, 0], across).wait_send()

        if first < chunks:
            at_distance(d, y_sent)
    for way, inside in ((0, a > 0), (1, a < na - 1)) if r_turned else ():

        @pl.when(inside)
        def _():
            view = r_cr.at[way, pl.ds(0, r_turned)]
            rcopy(view, view, c_s.at[way], c_r.at[0, 0], across).wait_send()

    view = r_z.at[pl.ds(0, na - 1)]
    rcopy(view, view, z_s.at[0], z_r.at[0, 0], across).wait_send()
    view = res.at[oc]
    rcopy(view, res_r, l_s.at[0], l_r.at[0], partner).wait_send()


def per_device(
    tokens,
    live_rows,
    expert_ids,
    gate_weights,
    norm_gain,
    expert_gate_up,
    expert_down,
    shared_gate_up,
    shared_down,
):
    step_count, row_count, model_width = tokens.shape
    n = lax.axis_size("expert")
    group = n // EXPERTS
    units = expert_down.shape[2]
    fb, s_wide = shared_gate_up.shape[1:]
    s_units = s_wide // 2
    nc = n // 2
    na = nc // 2
    half = model_width // 2
    rows = step_count * row_count
    pair = 2 * rows
    total = nc * pair
    y_rows = na * pair
    wide = half + LANES
    chunk = next(size for size in (512, 256, 128) if half % size == 0)
    chunks = half // chunk
    span = next(size for size in (128, 64, 32, 16) if fb % size == 0)
    window = -(-(fb + LANES - span) // LANES) * LANES
    dma = pltpu.SemaphoreType.DMA
    vmem = pltpu.VMEM
    whole = pl.BlockSpec(memory_space=pltpu.VMEM)
    anywhere = pl.BlockSpec(memory_space=pl.ANY)
    x_chunk = chunk if nc <= EXPERTS else half
    x_count = half // x_chunk
    x_turned = min(X_TURNED, x_count)
    r_turned = min(R_TURNED, chunks)
    z_places = 2 * na + 2 if na > 4 else na + 3
    return pl.pallas_call(
        functools.partial(layer_kernel, n, EXPERTS, group, chunk, window, x_chunk, x_turned, r_turned),
        out_shape=jax.ShapeDtypeStruct(tokens.shape, BF16),
        in_specs=[whole] * 5 + [anywhere] * 4,
        out_specs=whole,
        scratch_shapes=[
            vmem((rows, model_width), F32),
            vmem((2, rows, wide), F32),
            vmem((rows, wide), F32),
            vmem((2, total, wide), BF16),
            vmem((nc, pair, window), BF16),
            vmem((model_width, 2 * units), BF16),
            vmem((units, model_width), BF16),
            vmem((window, s_wide), BF16),
            vmem((fb, s_units), BF16),
            vmem((total, max(2 * units, GROUPED * chunk)), F32),
            vmem((total, units), BF16),
            vmem((2, total, s_units), F32),
            vmem((total, s_units), BF16),
            vmem((total, s_units), BF16),
            vmem((nc, pair, s_units), BF16),
            vmem((nc - 1, pair, s_units), BF16),
            vmem((2, total, s_units // 2), BF16),
            vmem((n, rows, fb), BF16),
            vmem((n, rows, fb), BF16),
            vmem((chunks, total, chunk), BF16),
            vmem((chunks, total, chunk), BF16),
            vmem((na, chunks, pair, chunk), BF16),
            vmem((na, chunks, pair, chunk), BF16),
            vmem((na, chunks, pair, chunk), BF16),
            vmem((z_places, chunks, pair, chunk), BF16),
            vmem((2, chunks, pair, chunk), BF16),
            vmem((chunks, pair, chunk), F32),
            vmem((na, chunks, pair, chunk), F32),
            vmem((2, chunks, rows, chunk), F32),
            vmem((chunks, rows, chunk), F32),
            dma((3 + x_count,)),
            dma((2,)),
            dma((1,)),
            dma((1,)),
            dma((2, 2, na)),
            dma((2,)),
            dma((na,)),
            dma((1,)),
            dma((nc, x_count)),
            dma((x_count,)),
            dma((4,)),
            dma((2,)),
            dma((2,)),
            dma((2,)),
            dma((1,)),
            dma((chunks,)),
            dma((2,)),
            dma((2, chunks)),
            dma((na,)),
            dma((na, chunks)),
            dma((1,)),
            dma((z_places, chunks)),
            dma((1,)),
            dma((chunks,)),
        ],
        compiler_params=pltpu.CompilerParams(
            collective_id=0, has_side_effects=True, vmem_limit_bytes=67_043_328
        ),
    )(
        tokens,
        live_rows.T,
        expert_ids,
        gate_weights,
        norm_gain,
        expert_gate_up,
        expert_down,
        shared_gate_up,
        jnp.swapaxes(shared_down, 1, 2),
    )


def solution(mesh):
    placed = (
        P(None, ("parts", "expert"), None),
        P(None, ("parts", "expert")),
        P(None, None, ("parts", "expert"), None),
        P(None, None, ("parts", "expert"), None),
        P(),
        P(None, "expert", None, None),
        P(None, "expert", None, None),
        P(None, "expert", None),
        P(None, None, "expert"),
    )
    return jax.shard_map(
        per_device,
        mesh=mesh,
        in_specs=placed,
        out_specs=P(None, ("parts", "expert"), None),
        check_vma=False,
    )
```

```python
import functools

import jax
import jax.numpy as jnp
from jax import lax
from jax.experimental import pallas as pl
from jax.experimental.pallas import tpu as pltpu
from jax.sharding import PartitionSpec as P

EXPERTS = 16
EPSILON = 1e-06
LANES = 128
X_TURNED = 3
R_TURNED = 2
GROUPED = 2
AT_PROJECT = 8
AT_ACROSS = 11
BF16 = jnp.bfloat16
F32 = jnp.float32


def dotted(left, right):
    return jnp.dot(left, right, preferred_element_type=F32)


def dotted_nt(left, right):
    return lax.dot_general(left, right, (((1,), (1,)), ((), ())), preferred_element_type=F32)


def layer_kernel(
    n,
    experts,
    group,
    chunk,
    window,
    x_chunk,
    x_turned,
    r_turned,
    tokens_ref,
    live_ref,
    ids_ref,
    gates_ref,
    gain_ref,
    gate_up_hbm,
    down_hbm,
    shared_up_hbm,
    shared_down_hbm,
    out_ref,
    acc,
    own_n,
    peer_n,
    x_all,
    x_win,
    gate_up,
    down,
    shared_up,
    shared_down,
    up_acc,
    hidden,
    sh_part,
    sh_send,
    sh_peer,
    sh_z,
    sh_zr,
    sh_hidden,
    so_send,
    so_recv,
    r_p,
    r_pr,
    r_y,
    r_yr,
    r_z,
    r_zr,
    r_cr,
    cross,
    keep,
    res,
    res_r,
    w_sem,
    n_sem,
    win_s,
    win_r,
    xz_s,
    xc_s,
    xy_s,
    xp_s,
    x_r,
    xp_r,
    h_sem,
    sp_sem,
    sz_sem,
    so_sem,
    p_s,
    p_r,
    c_s,
    c_r,
    y_s,
    y_r,
    z_s,
    z_r,
    l_s,
    l_r,
):
    nc = n // 2
    na = nc // 2
    me = lax.axis_index("expert")
    barrier = pltpu.get_barrier_semaphore()
    for d in range(1, n):
        pl.semaphore_signal(
            barrier,
            inc=1,
            device_id={"expert": lax.rem(me + d, n)},
            device_id_type=pl.DeviceIdType.MESH,
        )
    c = lax.rem(me, 2)
    chip = lax.div(me, 2)
    b = lax.rem(chip, 2)
    a = lax.div(chip, 2)
    slot = b * na + a
    oc = 1 - c
    steps, rows_dev, width = tokens_ref.shape
    half = width // 2
    rows = steps * rows_dev
    pair = 2 * rows
    total_rows = nc * pair
    y_rows = na * pair
    units = down.shape[0]
    s_units = sh_part.shape[2]
    fb = shared_down.shape[0]
    x_count = half // x_chunk
    chunks = half // chunk

    def dev(a_at, b_at, c_at):
        return {"expert": (2 * a_at + b_at) * 2 + c_at}

    partner = dev(a, b, oc)
    across = dev(a, 1 - b, c)
    below = dev(a - 1, b, c)
    above = dev(a + 1, b, c)

    def rcopy(src, dst, send, recv, to):
        return pltpu.make_async_remote_copy(
            src_ref=src,
            dst_ref=dst,
            send_sem=send,
            recv_sem=recv,
            device_id=to,
            device_id_type=pl.DeviceIdType.MESH,
        )

    def a_of(d):
        return lax.rem(a + d, na)

    def block(at):
        return pl.ds(pl.multiple_of(at * pair, pair), pair)

    loads = []
    offset = lax.rem(me, nc) * fb
    start = lax.div(offset, LANES) * LANES
    inner = pl.multiple_of(offset - start, 16)
    loads.append(
        pltpu.make_async_copy(
            shared_up_hbm.at[0], shared_up.at[pl.ds(inner, fb)], w_sem.at[0]
        )
    )
    for at in range(x_count):
        for side in range(2):
            piece = pl.ds(side * half + at * x_chunk, x_chunk)
            loads.append(
                pltpu.make_async_copy(
                    gate_up_hbm.at[0, 0, piece], gate_up.at[piece], w_sem.at[3 + at]
                )
            )
    loads.append(pltpu.make_async_copy(down_hbm.at[0, 0], down, w_sem.at[1]))
    down_load = loads[-1]
    loads.append(pltpu.make_async_copy(shared_down_hbm.at[0], shared_down, w_sem.at[2]))
    shared_down_load = loads[-1]

    def gate_up_wait(k):
        view = gate_up.at[pl.ds(0, 2 * x_chunk)]
        pltpu.make_async_copy(view, view, w_sem.at[3 + k]).wait()

    shared_up[...] = jnp.zeros_like(shared_up)

    for load in loads:
        load.start()

    lane = lax.broadcasted_iota(jnp.int32, (rows_dev, LANES), 1)
    row_at = lax.broadcasted_iota(jnp.int32, (rows_dev, LANES), 0)
    of_lane = lane & (experts - 1)
    level = lax.div(lane, experts)
    gain = gain_ref[...]
    for step in range(steps):
        h = tokens_ref[step].astype(F32)
        scaling = lax.rsqrt(jnp.mean(h * h, axis=-1, keepdims=True) + EPSILON)
        normed = (h * scaling * gain).astype(BF16).astype(F32)
        ids = ids_ref[0, step]
        gates = gates_ref[0, step]
        dense = jnp.zeros((rows_dev, LANES), F32)
        for k in range(ids.shape[1]):
            dense = dense + jnp.where(ids[:, k : k + 1] == of_lane, gates[:, k : k + 1], 0.0)
        dense = jnp.where(row_at < live_ref[:, step : step + 1], dense, 0.0)
        high = dense.astype(BF16).astype(F32)
        rest = dense - high
        mid = rest.astype(BF16).astype(F32)
        low = rest - mid
        coded = jnp.where(
            level == 0, high, jnp.where(level == 1, mid, jnp.where(level == 2, low, 0.0))
        )
        at = slice(step * rows_dev, (step + 1) * rows_dev)
        for side in range(2):
            own_n[side, at, :half] = normed[:, side * half : (side + 1) * half]
            own_n[side, at, half:] = coded

    pl.semaphore_wait(barrier, n - 1)

    swap = rcopy(own_n.at[oc], peer_n, n_sem.at[0], n_sem.at[1], partner)
    swap.start()
    swap.wait()
    mine = own_n[c]
    theirs = peer_n[...]
    first = jnp.where(c == 0, mine, theirs)
    second = jnp.where(c == 0, theirs, mine)
    x_all[c, block(slot)] = jnp.concatenate([first, second], axis=0).astype(BF16)

    def window_copy(i):
        lo = i * fb // LANES * LANES
        source = x_all.at[c, block(slot), pl.ds(lo, window)]
        return source, x_win.at[slot], win_r.at[0], c * nc + i

    def x_view(side, at, k):
        wide = x_chunk + (LANES if k == x_count - 1 else 0)
        return x_all.at[side, block(at), pl.ds(k * x_chunk, wide)]

    def x_push(at, k, send, to):
        view = x_view(c, at, k)
        rcopy(view, view, send, x_r.at[at, k], to).start()

    def x_twin(at, k):
        view = x_view(c, at, k)
        rcopy(view, view, xp_s.at[0], xp_r.at[k], partner).start()

    def x_arrived(at, k):
        view = x_view(c, at, k)
        rcopy(view, view, xp_s.at[0], x_r.at[at, k], partner).wait_recv()

    gate_down = lax.rem(a, 2) == 1
    gate_up_way = lax.rem(na - 1 - a, 2) == 1

    def x_steps(d, down_line, up_line):
        for way, line, gate in ((0, down_line, gate_down), (1, up_line, gate_up_way)):
            for step in (1, 2):
                if line:
                    inside = a >= step if way == 0 else a < na - step
                    goes = inside if d == 0 and step == 1 else inside & gate
                    yield way, step, goes, dev(a - step if way == 0 else a + step, b, c)

    def at_distance(d, body):
        if d == 0:
            body(a, True, True)
            return

        @pl.when(a + d < na)
        def _():
            body(a + d, True, False)

        @pl.when(a - d >= 0)
        def _():
            body(a - d, False, True)

    def x_along(d, k, gates=True):
        if not 0 <= k < x_count:
            return

        def one(source, down_line, up_line):
            at = b * na + source

            def handle():
                if d:
                    x_arrived(at, k)
                for way, step, goes, to in x_steps(d, down_line, up_line):

                    @pl.when(goes)
                    def _():
                        x_push(at, k, xz_s.at[way, step - 1, source], to)

                if d != 1 or k >= x_turned:
                    x_push(at, k, xy_s.at[source], across)
                x_twin(at, k)

            if d < 2:
                handle()
            else:
                gate = gate_down if down_line else gate_up_way
                pl.when(gate if gates else jnp.logical_not(gate))(handle)

        at_distance(d, one)

    def x_crossed(d, k):
        if not 0 <= k < x_count:
            return

        def one(source, down_line, up_line):
            at = (1 - b) * na + source
            x_arrived(at, k)
            if d == 0 and k < x_turned:
                for way, inside, to in ((0, a > 0, below), (1, a < na - 1, above)):

                    @pl.when(inside)
                    def _():
                        x_push(at, k, xc_s.at[way], to)

            x_twin(at, k)

        at_distance(d, one)

    def x_sent(d):
        def sent(sem, lo=0, hi=half + LANES):
            if lo < hi:
                view = x_all.at[c, block(0), pl.ds(lo, hi - lo)]
                rcopy(view, view, sem, x_r.at[0, 0], partner).wait_send()

        turned = half + LANES if x_turned == x_count else x_turned * x_chunk

        def one(source, down_line, up_line):
            for way, step, goes, _ in x_steps(d, down_line, up_line):

                @pl.when(goes)
                def _():
                    sent(xz_s.at[way, step - 1, source])

            if d == 0:
                for way, inside in ((0, a > 0), (1, a < na - 1)):

                    @pl.when(inside)
                    def _():
                        sent(xc_s.at[way], 0, turned)

            sent(xy_s.at[source], turned if d == 1 else 0)

        at_distance(d, one)

    s_half = s_units // 2

    def shared_project():
        loads[0].wait()
        rcopy(x_win, x_win, win_s.at[0], win_r.at[0], partner).wait_recv()
        features = x_win[...].reshape(total_rows, window)
        for side in range(2):
            for kind in range(2):
                cols = slice(kind * s_units + side * s_half, kind * s_units + (side + 1) * s_half)
                sh_part[side, :, kind * s_half : (kind + 1) * s_half] = dotted(
                    features, shared_up[:, cols]
                )
        sh_send[...] = sh_part[oc].astype(BF16)
        copy = rcopy(sh_send, sh_peer, sp_sem.at[0], sp_sem.at[1], partner)
        copy.start()
        return copy

    y_own = pl.ds(pl.multiple_of(b * y_rows, y_rows), y_rows)
    y_other = pl.ds(pl.multiple_of((1 - b) * y_rows, y_rows), y_rows)

    def shared_spread(copy):
        copy.wait()
        sh_part[0] = sh_part[c] + sh_peer[...].astype(F32)
        sh_z[...] = sh_part[0].astype(BF16).reshape(nc, pair, s_units)
        for d in range(1, nc):
            other = lax.rem(chip + d, nc)
            rcopy(
                sh_z.at[lax.rem(other, 2) * na + lax.div(other, 2)],
                sh_zr.at[d - 1],
                sz_sem.at[0],
                sz_sem.at[1],
                {"expert": other * 2 + c},
            ).start()

    others = pl.ds(0, (nc - 1) * pair)

    def shared_active():
        rcopy(sh_zr, sh_zr, sz_sem.at[0], sz_sem.at[1], partner).wait()
        total = sh_part[0, block(slot)]
        for d in range(1, nc):
            total = total + sh_zr[d - 1].astype(F32)
        sh_hidden[c, block(slot)] = (
            jax.nn.silu(total[:, :s_half]) * total[:, s_half:]
        ).astype(BF16)
        view = sh_hidden.at[c, block(slot)]
        for d in range(1, nc):
            to = {"expert": lax.rem(chip + d, nc) * 2 + c}
            rcopy(view, view, h_sem.at[0], h_sem.at[1], to).start()

    def shared_twin():
        view = sh_hidden.at[c, others]
        rcopy(view, view, h_sem.at[0], h_sem.at[1], partner).wait()
        view = sh_hidden.at[c]
        rcopy(view, view, h_sem.at[2], h_sem.at[3], partner).start()

    def shared_last():
        view = sh_hidden.at[c]
        rcopy(view, view, h_sem.at[2], h_sem.at[3], partner).wait()
        shared_down_load.wait()
        cols = dotted_nt(sh_hidden[0], shared_down[:, :s_half]) + dotted_nt(
            sh_hidden[1], shared_down[:, s_half:]
        )
        cols = cols.reshape(n, rows, fb).astype(BF16)
        for at in range(n):
            owner = 4 * (at // 2 % na) + 2 * (at // 2 // na) + at % 2
            so_send[lax.rem(owner - me + n, n)] = cols[at]
        for d in range(1, n):
            to = {"expert": lax.rem(me + d, n)}
            rcopy(so_send.at[d], so_recv.at[n - d], so_sem.at[0], so_sem.at[1], to).start()
        so_recv[0] = so_send[0]

    def shared_collect():
        view = so_recv.at[pl.ds(1, n - 1)]
        rcopy(view, view, so_sem.at[0], so_sem.at[1], partner).wait()

    def up_term(k, cols):
        at = k * x_chunk
        return dotted(x_all[0, :, at : at + x_chunk], gate_up[at : at + x_chunk, cols]) + dotted(
            x_all[1, :, at : at + x_chunk], gate_up[half + at : half + at + x_chunk, cols]
        )

    tile = min(256, units)

    def up_part(k):
        wide = x_chunk + (LANES if k == x_count - 1 else 0)
        view = x_all.at[oc, :, pl.ds(k * x_chunk, wide)]
        rcopy(view, view, xp_s.at[0], xp_r.at[k], partner).wait_recv()
        gate_up_wait(k)
        if k < x_count - 1:
            for at in range(2 * units // tile):
                cols = slice(at * tile, (at + 1) * tile)
                if k == 0:
                    up_acc[:, cols] = up_term(k, cols)
                else:
                    up_acc[:, cols] += up_term(k, cols)
            return
        for at in range(units // tile):
            gate_cols = slice(at * tile, (at + 1) * tile)
            up_cols = slice(units + at * tile, units + (at + 1) * tile)
            gate = up_term(k, gate_cols)
            up = up_term(k, up_cols)
            if k:
                gate = gate + up_acc[:, gate_cols]
                up = up + up_acc[:, up_cols]
            hidden[:, gate_cols] = (jax.nn.silu(gate) * up).astype(BF16)

    for k in range(x_count):
        x_along(0, k)
    for i in range(nc):
        source, target, recv, to = window_copy(i)

        @pl.when(to != me)
        def _():
            rcopy(source, target, win_s.at[0], recv, {"expert": to}).start()

        @pl.when(to == me)
        def _():
            pltpu.make_async_copy(source, target, recv).start()

    def gate_lag(d):
        return 3 * ((d - 1) // 2)

    def leaf_lag(d):
        return 0 if d < 2 else 3 * ((d - 2) // 2) + 3

    last_lag = leaf_lag(na - 1) + 4
    up_lag = last_lag + 2
    count = x_count + up_lag
    shared_copy = None
    for i in range(count):
        for d in range(1, na):
            x_along(d, i - gate_lag(d))
        x_crossed(0, i)
        for d in range(2, na):
            x_along(d, i - leaf_lag(d), False)
        if i == min(AT_PROJECT, count - 4):
            shared_copy = shared_project()
        if i == min(AT_ACROSS, count - 3):
            shared_spread(shared_copy)
        for d in range(1, na - 1):
            x_crossed(d, i - leaf_lag(d) - 4)
        x_crossed(na - 1, i - last_lag)
        if i >= up_lag:
            up_part(i - up_lag)

    expert = lax.div(me, group)
    codes = x_all[0, :, half:].astype(F32)
    wide = lax.broadcasted_iota(jnp.int32, (total_rows, LANES), 1) & (experts - 1)
    weight = jnp.sum(jnp.where(wide == expert, codes, 0.0), axis=1, keepdims=True)

    down_load.wait()

    def product(side, group):
        wide = chunk * len(group)
        cols = pl.ds(pl.multiple_of(side * half + group[0] * chunk, LANES), wide)
        return dotted(hidden[...], down[:, cols]) * weight

    def send_partner(group):
        sums = product(oc, group).astype(BF16)
        for place, j in enumerate(group):
            r_p[j] = sums[:, place * chunk : (place + 1) * chunk]
        for j in group:
            rcopy(r_p.at[j], r_pr.at[j], p_s.at[0], p_r.at[j], partner).start()

    def send_across(at, j):
        rcopy(r_y.at[at, j], r_yr.at[at, j], y_s.at[at], y_r.at[at, j], across).start()

    far = jnp.where(2 * a >= na, 0, na - 1)
    cross_rows = block((1 - b) * na + a)

    def own_part(group):
        up_acc[:, : chunk * len(group)] = product(c, group)
        for j in group:
            rcopy(r_p.at[j], r_pr.at[j], p_s.at[0], p_r.at[j], partner).wait_recv()
        for place, j in enumerate(group):
            cols = slice(place * chunk, (place + 1) * chunk)
            other = (up_acc[y_other, cols] + r_pr[j, y_other].astype(F32)).astype(BF16)
            for at in range(na):
                r_y[at, j] = other[at * pair : (at + 1) * pair]
        for place, j in enumerate(group):
            send_across(far, j)

            def beside(at, up_line, down_line):
                way, to = (1, above) if up_line else (0, below)
                rcopy(r_y.at[at, j], r_cr.at[way, j], c_s.at[way], c_r.at[way, j], to).start()

            if j < r_turned:
                at_distance(1, beside)
        for place, j in enumerate(group):
            cols = slice(place * chunk, (place + 1) * chunk)
            cross[j] = up_acc[cross_rows, cols] + r_pr[j, cross_rows].astype(F32)
            here = up_acc[y_own, cols] + r_pr[j, y_own].astype(F32)
            for at in range(na):
                keep[at, j] = here[at * pair : (at + 1) * pair]

    def join(j):
        for way, inside in ((1, a > 0), (0, a < na - 1)) if j < r_turned else ():

            @pl.when(inside)
            def _():
                view = r_cr.at[way, j]
                rcopy(view, view, c_s.at[0], c_r.at[way, j], across).wait_recv()
                cross[j] = cross[j] + r_cr[way, j].astype(F32)

        r_y[a, j] = cross[j].astype(BF16)
        send_across(a, j)

    def y_arrived(at, j):
        rcopy(r_y.at[at, j], r_yr.at[at, j], y_s.at[at], y_r.at[at, j], across).wait_recv()

    def z_place(step, place):
        if step == 1 or na > 4:
            return (step - 1) * (na + 1) + place
        return na + 1 + (place is na)

    def z_add(step, place, at, j):
        index = z_place(step, place)
        view = r_zr.at[index, j]
        rcopy(view, view, z_s.at[0], z_r.at[index, j], across).wait_recv()
        keep[at, j] = keep[at, j] + r_zr[index, j].astype(F32)

    def gate_even(up_line):
        return lax.rem(na - 1 - a if up_line else a, 2) == 0

    def leaf(up_line):
        return jnp.logical_not(gate_even(up_line))

    def z_pass(d, j, only=None):
        def one(at, up_line, down_line):
            if only is None:
                forward(at, up_line)
            else:
                pl.when(only(up_line))(lambda: forward(at, up_line))

        def forward(at, up_line):
            if d > 1 or j >= r_turned:
                y_arrived(at, j)
                keep[at, j] = keep[at, j] + r_yr[at, j].astype(F32)
            for step in (1, 2):
                if d + step < na:

                    @pl.when(gate_even(up_line) & (a >= step if up_line else a < na - step))
                    def _():
                        z_add(step, at, at, j)

            r_z[at, j] = keep[at, j].astype(BF16)
            last = na if not up_line else at

            def send(hop, place):
                to = dev(a + hop if up_line else a - hop, b, c)
                index = z_place(hop, place)
                rcopy(
                    r_z.at[at, j], r_zr.at[index, j], z_s.at[0], z_r.at[index, j], to
                ).start()

            if d == 1:
                send(1, last)
            else:
                even = gate_even(up_line)
                pl.when(even)(lambda: send(2, last if d == 2 else at))
                pl.when(jnp.logical_not(even))(lambda: send(1, at))

        at_distance(d, one)

    def collect(j):
        y_arrived(a, j)
        keep[a, j] = keep[a, j] + r_yr[a, j].astype(F32)
        for step in (1, 2):
            for place, inside, up_line in ((a, a >= step, True), (na, a < na - step, False)):
                if step == 2:
                    inside = inside & gate_even(up_line)

                @pl.when(inside)
                def _():
                    z_add(step, place, a, j)

        total = keep[a, j]
        res[0, j] = total[:rows]
        res[1, j] = total[rows:]
        rcopy(res.at[oc, j], res_r.at[j], l_s.at[0], l_r.at[j], partner).start()

    groups = [tuple(range(j, min(j + GROUPED, chunks))) for j in range(0, chunks, GROUPED)]
    send_partner(groups[0])
    for at, group in enumerate(groups):
        if at + 1 < len(groups):
            send_partner(groups[at + 1])
        own_part(group)
        for j in group:
            if j < r_turned:
                z_pass(1, j, leaf)
    for d in range(na - 2, 1, -1):

        def send_rest(at, up_line, down_line):
            @pl.when(at != far)
            def _():
                for j in range(chunks):
                    send_across(at, j)

        at_distance(d, send_rest)
    shared_active()
    for j in range(r_turned, chunks):
        at_distance(1, lambda at, up_line, down_line: send_across(at, j))
    for j in range(chunks):
        join(j)
    for d in range(na - 1, 2, -1):
        for j in range(chunks):
            z_pass(d, j)
    if na > 2:
        for j in range(chunks):
            z_pass(2, j, leaf)
    shared_twin()
    if na > 2:
        for j in range(chunks):
            z_pass(2, j, gate_even)
    shared_last()
    for j in range(chunks):
        z_pass(1, j, gate_even if j < r_turned else None)
    for j in range(chunks):
        collect(j)
    shared_collect()
    for j in range(chunks):
        rcopy(res.at[oc, j], res_r.at[j], l_s.at[0], l_r.at[j], partner).wait_recv()
        own_cols = pl.ds(pl.multiple_of(c * half + j * chunk, LANES), chunk)
        other_cols = pl.ds(pl.multiple_of(oc * half + j * chunk, LANES), chunk)
        acc[:, own_cols] = res[c, j]
        acc[:, other_cols] = res_r[j]
    for at in range(n):
        cols = slice(at * fb, (at + 1) * fb)
        acc[:, cols] = acc[:, cols] + so_recv[lax.rem(at - me + n, n)].astype(F32)
    row_of = lax.broadcasted_iota(jnp.int32, (rows_dev, width), 0)
    for step in range(steps):
        update = acc[step * rows_dev : (step + 1) * rows_dev]
        update = jnp.where(row_of < live_ref[:, step : step + 1], update, 0.0)
        out_ref[step] = (tokens_ref[step].astype(F32) + update).astype(BF16)
    @pl.when(lax.div(me, nc) == c)
    def _():
        view = x_win.at[pl.ds(0, nc - 1)]
        rcopy(view, view, win_s.at[0], win_r.at[0], partner).wait_send()

    @pl.when(lax.div(me, nc) != c)
    def _():
        rcopy(x_win, x_win, win_s.at[0], win_r.at[0], partner).wait_send()

    for d in range(na):
        x_sent(d)
    view = x_all.at[c]
    rcopy(view, view, xp_s.at[0], xp_r.at[0], partner).wait_send()
    rcopy(r_p, r_pr, p_s.at[0], p_r.at[0], partner).wait_send()
    for d in range(na):
        first = r_turned if d == 1 else 0

        def y_sent(at, up_line, down_line):
            view = r_y.at[at, pl.ds(first, chunks - first)]
            rcopy(view, view, y_s.at[at], y_r.at[0, 0], across).wait_send()

        if first < chunks:
            at_distance(d, y_sent)
    for way, inside in ((0, a > 0), (1, a < na - 1)) if r_turned else ():

        @pl.when(inside)
        def _():
            view = r_cr.at[way, pl.ds(0, r_turned)]
            rcopy(view, view, c_s.at[way], c_r.at[0, 0], across).wait_send()

    view = r_z.at[pl.ds(0, na - 1)]
    rcopy(view, view, z_s.at[0], z_r.at[0, 0], across).wait_send()
    view = res.at[oc]
    rcopy(view, res_r, l_s.at[0], l_r.at[0], partner).wait_send()


def per_device(
    tokens,
    live_rows,
    expert_ids,
    gate_weights,
    norm_gain,
    expert_gate_up,
    expert_down,
    shared_gate_up,
    shared_down,
):
    step_count, row_count, model_width = tokens.shape
    n = lax.axis_size("expert")
    group = n // EXPERTS
    units = expert_down.shape[2]
    fb, s_wide = shared_gate_up.shape[1:]
    s_units = s_wide // 2
    nc = n // 2
    na = nc // 2
    half = model_width // 2
    rows = step_count * row_count
    pair = 2 * rows
    total = nc * pair
    y_rows = na * pair
    wide = half + LANES
    chunk = next(size for size in (512, 256, 128) if half % size == 0)
    chunks = half // chunk
    span = next(size for size in (128, 64, 32, 16) if fb % size == 0)
    window = -(-(fb + LANES - span) // LANES) * LANES
    dma = pltpu.SemaphoreType.DMA
    vmem = pltpu.VMEM
    whole = pl.BlockSpec(memory_space=pltpu.VMEM)
    anywhere = pl.BlockSpec(memory_space=pl.ANY)
    x_chunk = chunk if nc <= EXPERTS else half
    x_count = half // x_chunk
    x_turned = min(X_TURNED, x_count)
    r_turned = min(R_TURNED, chunks)
    z_places = 2 * na + 2 if na > 4 else na + 3
    return pl.pallas_call(
        functools.partial(layer_kernel, n, EXPERTS, group, chunk, window, x_chunk, x_turned, r_turned),
        out_shape=jax.ShapeDtypeStruct(tokens.shape, BF16),
        in_specs=[whole] * 5 + [anywhere] * 4,
        out_specs=whole,
        scratch_shapes=[
            vmem((rows, model_width), F32),
            vmem((2, rows, wide), F32),
            vmem((rows, wide), F32),
            vmem((2, total, wide), BF16),
            vmem((nc, pair, window), BF16),
            vmem((model_width, 2 * units), BF16),
            vmem((units, model_width), BF16),
            vmem((window, s_wide), BF16),
            vmem((fb, s_units), BF16),
            vmem((total, max(2 * units, GROUPED * chunk)), F32),
            vmem((total, units), BF16),
            vmem((2, total, s_units), F32),
            vmem((total, s_units), BF16),
            vmem((total, s_units), BF16),
            vmem((nc, pair, s_units), BF16),
            vmem((nc - 1, pair, s_units), BF16),
            vmem((2, total, s_units // 2), BF16),
            vmem((n, rows, fb), BF16),
            vmem((n, rows, fb), BF16),
            vmem((chunks, total, chunk), BF16),
            vmem((chunks, total, chunk), BF16),
            vmem((na, chunks, pair, chunk), BF16),
            vmem((na, chunks, pair, chunk), BF16),
            vmem((na, chunks, pair, chunk), BF16),
            vmem((z_places, chunks, pair, chunk), BF16),
            vmem((2, chunks, pair, chunk), BF16),
            vmem((chunks, pair, chunk), F32),
            vmem((na, chunks, pair, chunk), F32),
            vmem((2, chunks, rows, chunk), F32),
            vmem((chunks, rows, chunk), F32),
            dma((3 + x_count,)),
            dma((2,)),
            dma((1,)),
            dma((1,)),
            dma((2, 2, na)),
            dma((2,)),
            dma((na,)),
            dma((1,)),
            dma((nc, x_count)),
            dma((x_count,)),
            dma((4,)),
            dma((2,)),
            dma((2,)),
            dma((2,)),
            dma((1,)),
            dma((chunks,)),
            dma((2,)),
            dma((2, chunks)),
            dma((na,)),
            dma((na, chunks)),
            dma((1,)),
            dma((z_places, chunks)),
            dma((1,)),
            dma((chunks,)),
        ],
        compiler_params=pltpu.CompilerParams(
            collective_id=0, has_side_effects=True, vmem_limit_bytes=67_043_328
        ),
    )(
        tokens,
        live_rows.T,
        expert_ids,
        gate_weights,
        norm_gain,
        expert_gate_up,
        expert_down,
        shared_gate_up,
        jnp.swapaxes(shared_down, 1, 2),
    )


def solution(mesh):
    placed = (
        P(None, ("parts", "expert"), None),
        P(None, ("parts", "expert")),
        P(None, None, ("parts", "expert"), None),
        P(None, None, ("parts", "expert"), None),
        P(),
        P(None, "expert", None, None),
        P(None, "expert", None, None),
        P(None, "expert", None),
        P(None, None, "expert"),
    )
    return jax.shard_map(
        per_device,
        mesh=mesh,
        in_specs=placed,
        out_specs=P(None, ("parts", "expert"), None),
        check_vma=False,
    )
```

```python
import functools

import jax
import jax.numpy as jnp
from jax import lax
from jax.experimental import pallas as pl
from jax.experimental.pallas import tpu as pltpu
from jax.sharding import PartitionSpec as P

EXPERTS = 16
EPSILON = 1e-06
LANES = 128
X_TURNED = 0
R_TURNED = 2
GROUPED = 2
AT_PROJECT = 8
AT_ACROSS = 11
BF16 = jnp.bfloat16
F32 = jnp.float32


def dotted(left, right):
    return jnp.dot(left, right, preferred_element_type=F32)


def dotted_nt(left, right):
    return lax.dot_general(left, right, (((1,), (1,)), ((), ())), preferred_element_type=F32)


def layer_kernel(
    n,
    experts,
    group,
    chunk,
    window,
    x_chunk,
    x_turned,
    r_turned,
    tokens_ref,
    live_ref,
    ids_ref,
    gates_ref,
    gain_ref,
    gate_up_hbm,
    down_hbm,
    shared_up_hbm,
    shared_down_hbm,
    out_ref,
    acc,
    own_n,
    peer_n,
    x_all,
    x_win,
    gate_up,
    down,
    shared_up,
    shared_down,
    up_acc,
    hidden,
    sh_part,
    sh_send,
    sh_peer,
    sh_z,
    sh_zr,
    sh_hidden,
    so_send,
    so_recv,
    r_p,
    r_pr,
    r_y,
    r_yr,
    r_z,
    r_zr,
    r_cr,
    cross,
    keep,
    res,
    res_r,
    w_sem,
    n_sem,
    win_s,
    win_r,
    xy_s,
    xp_s,
    x_r,
    xp_r,
    h_sem,
    sp_sem,
    sz_sem,
    so_sem,
    p_s,
    p_r,
    c_s,
    c_r,
    y_s,
    y_r,
    z_s,
    z_r,
    l_s,
    l_r,
):
    nc = n // 2
    na = nc // 2
    me = lax.axis_index("expert")
    barrier = pltpu.get_barrier_semaphore()
    for d in range(1, n):
        pl.semaphore_signal(
            barrier,
            inc=1,
            device_id={"expert": lax.rem(me + d, n)},
            device_id_type=pl.DeviceIdType.MESH,
        )
    c = lax.rem(me, 2)
    chip = lax.div(me, 2)
    b = lax.rem(chip, 2)
    a = lax.div(chip, 2)
    slot = b * na + a
    oc = 1 - c
    steps, rows_dev, width = tokens_ref.shape
    half = width // 2
    rows = steps * rows_dev
    pair = 2 * rows
    total_rows = nc * pair
    y_rows = na * pair
    units = down.shape[0]
    s_units = sh_part.shape[2]
    fb = shared_down.shape[0]
    x_count = half // x_chunk
    chunks = half // chunk

    def dev(a_at, b_at, c_at):
        return {"expert": (2 * a_at + b_at) * 2 + c_at}

    partner = dev(a, b, oc)
    across = dev(a, 1 - b, c)
    below = dev(a - 1, b, c)
    above = dev(a + 1, b, c)

    def rcopy(src, dst, send, recv, to):
        return pltpu.make_async_remote_copy(
            src_ref=src,
            dst_ref=dst,
            send_sem=send,
            recv_sem=recv,
            device_id=to,
            device_id_type=pl.DeviceIdType.MESH,
        )

    def a_of(d):
        return lax.rem(a + d, na)

    def block(at):
        return pl.ds(pl.multiple_of(at * pair, pair), pair)

    loads = []
    offset = lax.rem(me, nc) * fb
    start = lax.div(offset, LANES) * LANES
    inner = pl.multiple_of(offset - start, 16)
    loads.append(
        pltpu.make_async_copy(
            shared_up_hbm.at[0], shared_up.at[pl.ds(inner, fb)], w_sem.at[0]
        )
    )
    for at in range(x_count):
        for side in range(2):
            piece = pl.ds(side * half + at * x_chunk, x_chunk)
            loads.append(
                pltpu.make_async_copy(
                    gate_up_hbm.at[0, 0, piece], gate_up.at[piece], w_sem.at[3 + at]
                )
            )
    loads.append(pltpu.make_async_copy(down_hbm.at[0, 0], down, w_sem.at[1]))
    down_load = loads[-1]
    loads.append(pltpu.make_async_copy(shared_down_hbm.at[0], shared_down, w_sem.at[2]))
    shared_down_load = loads[-1]

    def gate_up_wait(k):
        view = gate_up.at[pl.ds(0, 2 * x_chunk)]
        pltpu.make_async_copy(view, view, w_sem.at[3 + k]).wait()

    shared_up[...] = jnp.zeros_like(shared_up)

    for load in loads:
        load.start()

    lane = lax.broadcasted_iota(jnp.int32, (rows_dev, LANES), 1)
    row_at = lax.broadcasted_iota(jnp.int32, (rows_dev, LANES), 0)
    of_lane = lane & (experts - 1)
    level = lax.div(lane, experts)
    gain = gain_ref[...]
    for step in range(steps):
        h = tokens_ref[step].astype(F32)
        scaling = lax.rsqrt(jnp.mean(h * h, axis=-1, keepdims=True) + EPSILON)
        normed = (h * scaling * gain).astype(BF16).astype(F32)
        ids = ids_ref[0, step]
        gates = gates_ref[0, step]
        dense = jnp.zeros((rows_dev, LANES), F32)
        for k in range(ids.shape[1]):
            dense = dense + jnp.where(ids[:, k : k + 1] == of_lane, gates[:, k : k + 1], 0.0)
        dense = jnp.where(row_at < live_ref[:, step : step + 1], dense, 0.0)
        high = dense.astype(BF16).astype(F32)
        rest = dense - high
        mid = rest.astype(BF16).astype(F32)
        low = rest - mid
        coded = jnp.where(
            level == 0, high, jnp.where(level == 1, mid, jnp.where(level == 2, low, 0.0))
        )
        at = slice(step * rows_dev, (step + 1) * rows_dev)
        for side in range(2):
            own_n[side, at, :half] = normed[:, side * half : (side + 1) * half]
            own_n[side, at, half:] = coded

    pl.semaphore_wait(barrier, n - 1)

    swap = rcopy(own_n.at[oc], peer_n, n_sem.at[0], n_sem.at[1], partner)
    swap.start()
    swap.wait()
    mine = own_n[c]
    theirs = peer_n[...]
    first = jnp.where(c == 0, mine, theirs)
    second = jnp.where(c == 0, theirs, mine)
    x_all[c, block(slot)] = jnp.concatenate([first, second], axis=0).astype(BF16)

    def window_copy(i):
        lo = i * fb // LANES * LANES
        source = x_all.at[c, block(slot), pl.ds(lo, window)]
        return source, x_win.at[slot], win_r.at[0], c * nc + i

    def x_view(side, at, k):
        wide = x_chunk + (LANES if k == x_count - 1 else 0)
        return x_all.at[side, block(at), pl.ds(k * x_chunk, wide)]

    def x_push(at, k, send, to):
        view = x_view(c, at, k)
        rcopy(view, view, send, x_r.at[at, k], to).start()

    def x_twin(at, k):
        view = x_view(c, at, k)
        rcopy(view, view, xp_s.at[0], xp_r.at[k], partner).start()

    def x_arrived(at, k):
        view = x_view(c, at, k)
        rcopy(view, view, xp_s.at[0], x_r.at[at, k], partner).wait_recv()

    gate_down = lax.rem(a, 2) == 1
    gate_up_way = lax.rem(na - 1 - a, 2) == 1

    def x_steps(d, down_line, up_line):
        for way, line, gate in ((0, down_line, gate_down), (1, up_line, gate_up_way)):
            for step in (1, 2):
                if line:
                    inside = a >= step if way == 0 else a < na - step
                    goes = inside if d == 0 and step == 1 else inside & gate
                    yield way, step, goes, dev(a - step if way == 0 else a + step, b, c)

    def at_distance(d, body):
        if d == 0:
            body(a, True, True)
            return

        @pl.when(a + d < na)
        def _():
            body(a + d, True, False)

        @pl.when(a - d >= 0)
        def _():
            body(a - d, False, True)

    def x_along(d, k, gates=True):
        if not 0 <= k < x_count:
            return

        def one(source, down_line, up_line):
            at = b * na + source

            def handle():
                if d:
                    x_arrived(at, k)
                for way, step, goes, to in x_steps(d, down_line, up_line):

                    @pl.when(goes)
                    def _():
                        x_push(at, k, xy_s.at[0], to)

                if d != 1 or k >= x_turned:
                    x_push(at, k, xy_s.at[0], across)
                x_twin(at, k)

            if d < 2:
                handle()
            else:
                gate = gate_down if down_line else gate_up_way
                pl.when(gate if gates else jnp.logical_not(gate))(handle)

        at_distance(d, one)

    def x_crossed(d, k):
        if not 0 <= k < x_count:
            return

        def one(source, down_line, up_line):
            at = (1 - b) * na + source
            x_arrived(at, k)
            if d == 0 and k < x_turned:
                for way, inside, to in ((0, a > 0, below), (1, a < na - 1, above)):

                    @pl.when(inside)
                    def _():
                        x_push(at, k, xy_s.at[0], to)

            x_twin(at, k)

        at_distance(d, one)

    def x_sent(at):
        blocks = na
        for step in (1, 2):
            blocks += (at >= step) * (1 if step == 1 else at % 2)
            blocks += (at < na - step) * (1 if step == 1 else (na - 1 - at) % 2)
            if at % 2:
                blocks += (na - 1 - at) * (at >= step)
            if (na - 1 - at) % 2:
                blocks += at * (at < na - step)
        return blocks

    s_half = s_units // 2

    def shared_project():
        loads[0].wait()
        rcopy(x_win, x_win, win_s.at[0], win_r.at[0], partner).wait_recv()
        features = x_win[...].reshape(total_rows, window)
        for side in range(2):
            for kind in range(2):
                cols = slice(kind * s_units + side * s_half, kind * s_units + (side + 1) * s_half)
                sh_part[side, :, kind * s_half : (kind + 1) * s_half] = dotted(
                    features, shared_up[:, cols]
                )
        sh_send[...] = sh_part[oc].astype(BF16)
        copy = rcopy(sh_send, sh_peer, sp_sem.at[0], sp_sem.at[1], partner)
        copy.start()
        return copy

    y_own = pl.ds(pl.multiple_of(b * y_rows, y_rows), y_rows)
    y_other = pl.ds(pl.multiple_of((1 - b) * y_rows, y_rows), y_rows)

    def shared_spread(copy):
        copy.wait()
        sh_part[0] = sh_part[c] + sh_peer[...].astype(F32)
        sh_z[...] = sh_part[0].astype(BF16).reshape(nc, pair, s_units)
        for d in range(1, nc):
            other = lax.rem(chip + d, nc)
            rcopy(
                sh_z.at[lax.rem(other, 2) * na + lax.div(other, 2)],
                sh_zr.at[d - 1],
                sz_sem.at[0],
                sz_sem.at[1],
                {"expert": other * 2 + c},
            ).start()

    others = pl.ds(0, (nc - 1) * pair)

    def shared_active():
        rcopy(sh_zr, sh_zr, sz_sem.at[0], sz_sem.at[1], partner).wait()
        total = sh_part[0, block(slot)]
        for d in range(1, nc):
            total = total + sh_zr[d - 1].astype(F32)
        sh_hidden[c, block(slot)] = (
            jax.nn.silu(total[:, :s_half]) * total[:, s_half:]
        ).astype(BF16)
        view = sh_hidden.at[c, block(slot)]
        for d in range(1, nc):
            to = {"expert": lax.rem(chip + d, nc) * 2 + c}
            rcopy(view, view, h_sem.at[0], h_sem.at[1], to).start()

    def shared_twin():
        view = sh_hidden.at[c, others]
        rcopy(view, view, h_sem.at[0], h_sem.at[1], partner).wait()
        view = sh_hidden.at[c]
        rcopy(view, view, h_sem.at[2], h_sem.at[3], partner).start()

    def shared_last():
        view = sh_hidden.at[c]
        rcopy(view, view, h_sem.at[2], h_sem.at[3], partner).wait()
        shared_down_load.wait()
        cols = dotted_nt(sh_hidden[0], shared_down[:, :s_half]) + dotted_nt(
            sh_hidden[1], shared_down[:, s_half:]
        )
        cols = cols.reshape(n, rows, fb).astype(BF16)
        for at in range(n):
            owner = 4 * (at // 2 % na) + 2 * (at // 2 // na) + at % 2
            so_send[lax.rem(owner - me + n, n)] = cols[at]
        for d in range(1, n):
            to = {"expert": lax.rem(me + d, n)}
            rcopy(so_send.at[d], so_recv.at[n - d], so_sem.at[0], so_sem.at[1], to).start()
        so_recv[0] = so_send[0]

    def shared_collect():
        view = so_recv.at[pl.ds(1, n - 1)]
        rcopy(view, view, so_sem.at[0], so_sem.at[1], partner).wait()

    def up_term(k, cols):
        at = k * x_chunk
        return dotted(x_all[0, :, at : at + x_chunk], gate_up[at : at + x_chunk, cols]) + dotted(
            x_all[1, :, at : at + x_chunk], gate_up[half + at : half + at + x_chunk, cols]
        )

    tile = min(256, units)

    def up_part(k):
        wide = x_chunk + (LANES if k == x_count - 1 else 0)
        view = x_all.at[oc, :, pl.ds(k * x_chunk, wide)]
        rcopy(view, view, xp_s.at[0], xp_r.at[k], partner).wait_recv()
        gate_up_wait(k)
        if k < x_count - 1:
            for at in range(2 * units // tile):
                cols = slice(at * tile, (at + 1) * tile)
                if k == 0:
                    up_acc[:, cols] = up_term(k, cols)
                else:
                    up_acc[:, cols] += up_term(k, cols)
            return
        for at in range(units // tile):
            gate_cols = slice(at * tile, (at + 1) * tile)
            up_cols = slice(units + at * tile, units + (at + 1) * tile)
            gate = up_term(k, gate_cols)
            up = up_term(k, up_cols)
            if k:
                gate = gate + up_acc[:, gate_cols]
                up = up + up_acc[:, up_cols]
            hidden[:, gate_cols] = (jax.nn.silu(gate) * up).astype(BF16)

    for k in range(x_count):
        x_along(0, k)
    for i in range(nc):
        source, target, recv, to = window_copy(i)

        @pl.when(to != me)
        def _():
            rcopy(source, target, win_s.at[0], recv, {"expert": to}).start()

        @pl.when(to == me)
        def _():
            pltpu.make_async_copy(source, target, recv).start()

    def gate_lag(d):
        return 3 * ((d - 1) // 2)

    def leaf_lag(d):
        return 0 if d < 2 else 3 * ((d - 2) // 2) + 3

    last_lag = leaf_lag(na - 1) + 4
    up_lag = last_lag + 2
    count = x_count + up_lag
    shared_copy = None
    for i in range(count):
        for d in range(1, na):
            x_along(d, i - gate_lag(d))
        x_crossed(0, i)
        for d in range(2, na):
            x_along(d, i - leaf_lag(d), False)
        if i == min(AT_PROJECT, count - 4):
            shared_copy = shared_project()
        if i == min(AT_ACROSS, count - 3):
            shared_spread(shared_copy)
        for d in range(1, na - 1):
            x_crossed(d, i - leaf_lag(d) - 4)
        x_crossed(na - 1, i - last_lag)
        if i >= up_lag:
            up_part(i - up_lag)

    expert = lax.div(me, group)
    codes = x_all[0, :, half:].astype(F32)
    wide = lax.broadcasted_iota(jnp.int32, (total_rows, LANES), 1) & (experts - 1)
    weight = jnp.sum(jnp.where(wide == expert, codes, 0.0), axis=1, keepdims=True)

    down_load.wait()

    def paired(j):
        return pl.ds(j, min(2, chunks - j))

    def product(side, group):
        wide = chunk * len(group)
        cols = pl.ds(pl.multiple_of(side * half + group[0] * chunk, LANES), wide)
        return dotted(hidden[...], down[:, cols]) * weight

    def send_partner(group):
        sums = product(oc, group).astype(BF16)
        for place, j in enumerate(group):
            r_p[j] = sums[:, place * chunk : (place + 1) * chunk]
        for j in group:
            rcopy(r_p.at[j], r_pr.at[j], p_s.at[0], p_r.at[j // 2], partner).start()

    def send_across(at, j, send=0):
        rcopy(r_y.at[at, j], r_yr.at[at, j], y_s.at[send], y_r.at[at, j // 2], across).start()

    far = jnp.where(2 * a >= na, 0, na - 1)
    cross_rows = block((1 - b) * na + a)

    def own_part(group):
        up_acc[:, : chunk * len(group)] = product(c, group)
        for j in group[::2]:
            view = r_pr.at[paired(j)]
            rcopy(view, view, p_s.at[0], p_r.at[j // 2], partner).wait_recv()
        for place, j in enumerate(group):
            cols = slice(place * chunk, (place + 1) * chunk)
            other = (up_acc[y_other, cols] + r_pr[j, y_other].astype(F32)).astype(BF16)
            for at in range(na):
                r_y[at, j] = other[at * pair : (at + 1) * pair]
        for place, j in enumerate(group):
            send_across(far, j)

            def beside(at, up_line, down_line):
                way, to = (1, above) if up_line else (0, below)
                rcopy(r_y.at[at, j], r_cr.at[way, j], c_s.at[0], c_r.at[way], to).start()

            if j < r_turned:
                at_distance(1, beside)
        for place, j in enumerate(group):
            cols = slice(place * chunk, (place + 1) * chunk)
            cross[j] = up_acc[cross_rows, cols] + r_pr[j, cross_rows].astype(F32)
            here = up_acc[y_own, cols] + r_pr[j, y_own].astype(F32)
            for at in range(na):
                keep[at, j] = here[at * pair : (at + 1) * pair]

    def join(j):
        for way, inside in ((1, a > 0), (0, a < na - 1)) if j < r_turned else ():

            @pl.when(inside)
            def _():
                if j == 0:
                    view = r_cr.at[way, pl.ds(0, r_turned)]
                    rcopy(view, view, c_s.at[0], c_r.at[way], across).wait_recv()
                cross[j] = cross[j] + r_cr[way, j].astype(F32)

        r_y[a, j] = cross[j].astype(BF16)
        send_across(a, j)

    def y_arrived(at, j):
        if j % 2 == 0:
            view = r_yr.at[at, paired(j)]
            rcopy(view, view, y_s.at[0], y_r.at[at, j // 2], across).wait_recv()

    def z_place(step, place):
        if step == 1 or na > 4:
            return (step - 1) * (na + 1) + place
        return na + 1 + (place is na)

    def z_add(step, place, at, j):
        index = z_place(step, place)
        if j % 2 == 0:
            view = r_zr.at[index, paired(j)]
            rcopy(view, view, z_s.at[0], z_r.at[index, j // 2], across).wait_recv()
        keep[at, j] = keep[at, j] + r_zr[index, j].astype(F32)

    def gate_even(up_line):
        return lax.rem(na - 1 - a if up_line else a, 2) == 0

    def leaf(up_line):
        return jnp.logical_not(gate_even(up_line))

    def z_pass(d, j, only=None):
        def one(at, up_line, down_line):
            if only is None:
                forward(at, up_line)
            else:
                pl.when(only(up_line))(lambda: forward(at, up_line))

        def forward(at, up_line):
            if d > 1 or j >= r_turned:
                y_arrived(at, j)
                keep[at, j] = keep[at, j] + r_yr[at, j].astype(F32)
            for step in (1, 2):
                if d + step < na:

                    @pl.when(gate_even(up_line) & (a >= step if up_line else a < na - step))
                    def _():
                        z_add(step, at, at, j)

            r_z[at, j] = keep[at, j].astype(BF16)
            last = na if not up_line else at

            def send(hop, place):
                to = dev(a + hop if up_line else a - hop, b, c)
                index = z_place(hop, place)
                rcopy(
                    r_z.at[at, j], r_zr.at[index, j], z_s.at[0], z_r.at[index, j // 2], to
                ).start()

            if d == 1:
                send(1, last)
            else:
                even = gate_even(up_line)
                pl.when(even)(lambda: send(2, last if d == 2 else at))
                pl.when(jnp.logical_not(even))(lambda: send(1, at))

        at_distance(d, one)

    def collect(j):
        y_arrived(a, j)
        keep[a, j] = keep[a, j] + r_yr[a, j].astype(F32)
        for step in (1, 2):
            for place, inside, up_line in ((a, a >= step, True), (na, a < na - step, False)):
                if step == 2:
                    inside = inside & gate_even(up_line)

                @pl.when(inside)
                def _():
                    z_add(step, place, a, j)

        total = keep[a, j]
        res[0, j] = total[:rows]
        res[1, j] = total[rows:]
        rcopy(res.at[oc, j], res_r.at[j], l_s.at[0], l_r.at[j // 2], partner).start()

    groups = [tuple(range(j, min(j + GROUPED, chunks))) for j in range(0, chunks, GROUPED)]
    send_partner(groups[0])
    for at, group in enumerate(groups):
        if at + 1 < len(groups):
            send_partner(groups[at + 1])
        own_part(group)
        for j in group:
            if j < r_turned:
                z_pass(1, j, leaf)
    for d in range(na - 2, 1, -1):

        def send_rest(at, up_line, down_line):
            @pl.when(at != far)
            def _():
                for j in range(chunks):
                    send_across(at, j)

        at_distance(d, send_rest)
    shared_active()
    for j in range(r_turned, chunks):
        at_distance(1, lambda at, up_line, down_line: send_across(at, j, 1))
    for j in range(chunks):
        join(j)
    for d in range(na - 1, 2, -1):
        for j in range(chunks):
            z_pass(d, j)
    if na > 2:
        for j in range(chunks):
            z_pass(2, j, leaf)
    shared_twin()
    if na > 2:
        for j in range(chunks):
            z_pass(2, j, gate_even)
    shared_last()
    for j in range(chunks):
        z_pass(1, j, gate_even if j < r_turned else None)
    for j in range(chunks):
        collect(j)
    shared_collect()
    for j in range(chunks):
        if j % 2 == 0:
            view = res_r.at[paired(j)]
            rcopy(view, view, l_s.at[0], l_r.at[j // 2], partner).wait_recv()
        own_cols = pl.ds(pl.multiple_of(c * half + j * chunk, LANES), chunk)
        other_cols = pl.ds(pl.multiple_of(oc * half + j * chunk, LANES), chunk)
        acc[:, own_cols] = res[c, j]
        acc[:, other_cols] = res_r[j]
    for at in range(n):
        cols = slice(at * fb, (at + 1) * fb)
        acc[:, cols] = acc[:, cols] + so_recv[lax.rem(at - me + n, n)].astype(F32)
    row_of = lax.broadcasted_iota(jnp.int32, (rows_dev, width), 0)
    for step in range(steps):
        update = acc[step * rows_dev : (step + 1) * rows_dev]
        update = jnp.where(row_of < live_ref[:, step : step + 1], update, 0.0)
        out_ref[step] = (tokens_ref[step].astype(F32) + update).astype(BF16)
    @pl.when(lax.div(me, nc) == c)
    def _():
        view = x_win.at[pl.ds(0, nc - 1)]
        rcopy(view, view, win_s.at[0], win_r.at[0], partner).wait_send()

    @pl.when(lax.div(me, nc) != c)
    def _():
        rcopy(x_win, x_win, win_s.at[0], win_r.at[0], partner).wait_send()

    for at in range(na):

        @pl.when(a == at)
        def _():
            left = x_sent(at)
            while left:
                some = min(left, nc)
                view = x_all.at[c, pl.ds(0, some * pair)]
                rcopy(view, view, xy_s.at[0], x_r.at[0, 0], partner).wait_send()
                left -= some

    view = x_all.at[c]
    rcopy(view, view, xp_s.at[0], xp_r.at[0], partner).wait_send()
    rcopy(r_p, r_pr, p_s.at[0], p_r.at[0], partner).wait_send()
    for at in range(na):
        beside = (at > 0) + (at < na - 1)

        @pl.when(a == at)
        def _():
            if r_turned:
                view = r_y.at[pl.ds(0, beside), pl.ds(0, r_turned)]
                rcopy(view, view, c_s.at[0], c_r.at[0], across).wait_send()
            view = r_y.at[pl.ds(0, na - beside)]
            rcopy(view, view, y_s.at[0], y_r.at[0, 0], across).wait_send()
            if r_turned < chunks:
                view = r_y.at[pl.ds(0, beside), pl.ds(0, chunks - r_turned)]
                rcopy(view, view, y_s.at[1], y_r.at[0, 0], across).wait_send()

    view = r_z.at[pl.ds(0, na - 1)]
    rcopy(view, view, z_s.at[0], z_r.at[0, 0], across).wait_send()
    view = res.at[oc]
    rcopy(view, res_r, l_s.at[0], l_r.at[0], partner).wait_send()


def per_device(
    tokens,
    live_rows,
    expert_ids,
    gate_weights,
    norm_gain,
    expert_gate_up,
    expert_down,
    shared_gate_up,
    shared_down,
):
    step_count, row_count, model_width = tokens.shape
    n = lax.axis_size("expert")
    group = n // EXPERTS
    units = expert_down.shape[2]
    fb, s_wide = shared_gate_up.shape[1:]
    s_units = s_wide // 2
    nc = n // 2
    na = nc // 2
    half = model_width // 2
    rows = step_count * row_count
    pair = 2 * rows
    total = nc * pair
    y_rows = na * pair
    wide = half + LANES
    chunk = next(size for size in (512, 256, 128) if half % size == 0)
    chunks = half // chunk
    span = next(size for size in (128, 64, 32, 16) if fb % size == 0)
    window = -(-(fb + LANES - span) // LANES) * LANES
    dma = pltpu.SemaphoreType.DMA
    vmem = pltpu.VMEM
    whole = pl.BlockSpec(memory_space=pltpu.VMEM)
    anywhere = pl.BlockSpec(memory_space=pl.ANY)
    x_chunk = chunk if nc <= EXPERTS else half
    x_count = half // x_chunk
    x_turned = min(X_TURNED, x_count)
    r_turned = min(R_TURNED, chunks)
    pairs = (chunks + 1) // 2
    z_places = 2 * na + 2 if na > 4 else na + 3
    return pl.pallas_call(
        functools.partial(layer_kernel, n, EXPERTS, group, chunk, window, x_chunk, x_turned, r_turned),
        out_shape=jax.ShapeDtypeStruct(tokens.shape, BF16),
        in_specs=[whole] * 5 + [anywhere] * 4,
        out_specs=whole,
        scratch_shapes=[
            vmem((rows, model_width), F32),
            vmem((2, rows, wide), F32),
            vmem((rows, wide), F32),
            vmem((2, total, wide), BF16),
            vmem((nc, pair, window), BF16),
            vmem((model_width, 2 * units), BF16),
            vmem((units, model_width), BF16),
            vmem((window, s_wide), BF16),
            vmem((fb, s_units), BF16),
            vmem((total, max(2 * units, GROUPED * chunk)), F32),
            vmem((total, units), BF16),
            vmem((2, total, s_units), F32),
            vmem((total, s_units), BF16),
            vmem((total, s_units), BF16),
            vmem((nc, pair, s_units), BF16),
            vmem((nc - 1, pair, s_units), BF16),
            vmem((2, total, s_units // 2), BF16),
            vmem((n, rows, fb), BF16),
            vmem((n, rows, fb), BF16),
            vmem((chunks, total, chunk), BF16),
            vmem((chunks, total, chunk), BF16),
            vmem((na, chunks, pair, chunk), BF16),
            vmem((na, chunks, pair, chunk), BF16),
            vmem((na, chunks, pair, chunk), BF16),
            vmem((z_places, chunks, pair, chunk), BF16),
            vmem((2, chunks, pair, chunk), BF16),
            vmem((chunks, pair, chunk), F32),
            vmem((na, chunks, pair, chunk), F32),
            vmem((2, chunks, rows, chunk), F32),
            vmem((chunks, rows, chunk), F32),
            dma((3 + x_count,)),
            dma((2,)),
            dma((1,)),
            dma((1,)),
            dma((1,)),
            dma((1,)),
            dma((nc, x_count)),
            dma((x_count,)),
            dma((4,)),
            dma((2,)),
            dma((2,)),
            dma((2,)),
            dma((1,)),
            dma((pairs,)),
            dma((1,)),
            dma((2,)),
            dma((2,)),
            dma((na, pairs)),
            dma((1,)),
            dma((z_places, pairs)),
            dma((1,)),
            dma((pairs,)),
        ],
        compiler_params=pltpu.CompilerParams(
            collective_id=0, has_side_effects=True, vmem_limit_bytes=67_043_328
        ),
    )(
        tokens,
        live_rows.T,
        expert_ids,
        gate_weights,
        norm_gain,
        expert_gate_up,
        expert_down,
        shared_gate_up,
        jnp.swapaxes(shared_down, 1, 2),
    )


def solution(mesh):
    placed = (
        P(None, ("parts", "expert"), None),
        P(None, ("parts", "expert")),
        P(None, None, ("parts", "expert"), None),
        P(None, None, ("parts", "expert"), None),
        P(),
        P(None, "expert", None, None),
        P(None, "expert", None, None),
        P(None, "expert", None),
        P(None, None, "expert"),
    )
    return jax.shard_map(
        per_device,
        mesh=mesh,
        in_specs=placed,
        out_specs=P(None, ("parts", "expert"), None),
        check_vma=False,
    )
```

```python
import functools

import jax
import jax.numpy as jnp
from jax import lax
from jax.experimental import pallas as pl
from jax.experimental.pallas import tpu as pltpu
from jax.sharding import PartitionSpec as P

EXPERTS = 16
EPSILON = 1e-06
LANES = 128
X_TURNED = 0
R_TURNED = 2
GROUPED = 2
AT_PROJECT = 8
AT_ACROSS = 11
BF16 = jnp.bfloat16
F32 = jnp.float32


def dotted(left, right):
    return jnp.dot(left, right, preferred_element_type=F32)


def dotted_nt(left, right):
    return lax.dot_general(left, right, (((1,), (1,)), ((), ())), preferred_element_type=F32)


def layer_kernel(
    n,
    experts,
    group,
    chunk,
    window,
    x_chunk,
    x_turned,
    r_turned,
    tokens_ref,
    live_ref,
    ids_ref,
    gates_ref,
    gain_ref,
    gate_up_hbm,
    down_hbm,
    shared_up_hbm,
    shared_down_hbm,
    out_ref,
    acc,
    own_n,
    peer_n,
    x_all,
    x_win,
    gate_up,
    down,
    shared_up,
    shared_down,
    up_acc,
    hidden,
    sh_part,
    sh_send,
    sh_peer,
    sh_z,
    sh_zr,
    sh_hidden,
    so_send,
    so_recv,
    r_p,
    r_pr,
    r_y,
    r_yr,
    r_z,
    r_zr,
    r_cr,
    cross,
    keep,
    res,
    res_r,
    w_sem,
    n_sem,
    win_s,
    win_r,
    xy_s,
    xp_s,
    x_r,
    xp_r,
    h_sem,
    sp_sem,
    sz_sem,
    so_sem,
    p_s,
    p_r,
    c_s,
    c_r,
    y_s,
    y_r,
    z_s,
    z_r,
    l_s,
    l_r,
):
    nc = n // 2
    na = nc // 2
    me = lax.axis_index("expert")
    barrier = pltpu.get_barrier_semaphore()
    for d in range(1, n):
        pl.semaphore_signal(
            barrier,
            inc=1,
            device_id={"expert": lax.rem(me + d, n)},
            device_id_type=pl.DeviceIdType.MESH,
        )
    c = lax.rem(me, 2)
    chip = lax.div(me, 2)
    b = lax.rem(chip, 2)
    a = lax.div(chip, 2)
    slot = b * na + a
    oc = 1 - c
    steps, rows_dev, width = tokens_ref.shape
    half = width // 2
    rows = steps * rows_dev
    pair = 2 * rows
    total_rows = nc * pair
    y_rows = na * pair
    units = down.shape[0]
    s_units = sh_part.shape[2]
    fb = shared_down.shape[0]
    x_count = half // x_chunk
    chunks = half // chunk

    def dev(a_at, b_at, c_at):
        return {"expert": (2 * a_at + b_at) * 2 + c_at}

    partner = dev(a, b, oc)
    across = dev(a, 1 - b, c)
    below = dev(a - 1, b, c)
    above = dev(a + 1, b, c)

    def rcopy(src, dst, send, recv, to):
        return pltpu.make_async_remote_copy(
            src_ref=src,
            dst_ref=dst,
            send_sem=send,
            recv_sem=recv,
            device_id=to,
            device_id_type=pl.DeviceIdType.MESH,
        )

    def a_of(d):
        return lax.rem(a + d, na)

    def block(at):
        return pl.ds(pl.multiple_of(at * pair, pair), pair)

    loads = []
    offset = lax.rem(me, nc) * fb
    start = lax.div(offset, LANES) * LANES
    inner = pl.multiple_of(offset - start, 16)
    loads.append(
        pltpu.make_async_copy(
            shared_up_hbm.at[0], shared_up.at[pl.ds(inner, fb)], w_sem.at[0]
        )
    )
    for at in range(x_count):
        for side in range(2):
            piece = pl.ds(side * half + at * x_chunk, x_chunk)
            loads.append(
                pltpu.make_async_copy(
                    gate_up_hbm.at[0, 0, piece], gate_up.at[piece], w_sem.at[3 + at]
                )
            )
    loads.append(pltpu.make_async_copy(down_hbm.at[0, 0], down, w_sem.at[1]))
    down_load = loads[-1]
    loads.append(pltpu.make_async_copy(shared_down_hbm.at[0], shared_down, w_sem.at[2]))
    shared_down_load = loads[-1]

    def gate_up_wait(k):
        view = gate_up.at[pl.ds(0, 2 * x_chunk)]
        pltpu.make_async_copy(view, view, w_sem.at[3 + k]).wait()

    shared_up[...] = jnp.zeros_like(shared_up)

    for load in loads:
        load.start()

    lane = lax.broadcasted_iota(jnp.int32, (rows_dev, LANES), 1)
    row_at = lax.broadcasted_iota(jnp.int32, (rows_dev, LANES), 0)
    of_lane = lane & (experts - 1)
    level = lax.div(lane, experts)
    gain = gain_ref[...]
    for step in range(steps):
        h = tokens_ref[step].astype(F32)
        scaling = lax.rsqrt(jnp.mean(h * h, axis=-1, keepdims=True) + EPSILON)
        normed = (h * scaling * gain).astype(BF16).astype(F32)
        ids = ids_ref[0, step]
        gates = gates_ref[0, step]
        dense = jnp.zeros((rows_dev, LANES), F32)
        for k in range(ids.shape[1]):
            dense = dense + jnp.where(ids[:, k : k + 1] == of_lane, gates[:, k : k + 1], 0.0)
        dense = jnp.where(row_at < live_ref[:, step : step + 1], dense, 0.0)
        high = dense.astype(BF16).astype(F32)
        rest = dense - high
        mid = rest.astype(BF16).astype(F32)
        low = rest - mid
        coded = jnp.where(
            level == 0, high, jnp.where(level == 1, mid, jnp.where(level == 2, low, 0.0))
        )
        at = slice(step * rows_dev, (step + 1) * rows_dev)
        for side in range(2):
            own_n[side, at, :half] = normed[:, side * half : (side + 1) * half]
            own_n[side, at, half:] = coded

    pl.semaphore_wait(barrier, n - 1)

    swap = rcopy(own_n.at[oc], peer_n, n_sem.at[0], n_sem.at[1], partner)
    swap.start()
    swap.wait()
    mine = own_n[c]
    theirs = peer_n[...]
    first = jnp.where(c == 0, mine, theirs)
    second = jnp.where(c == 0, theirs, mine)
    x_all[c, block(slot)] = jnp.concatenate([first, second], axis=0).astype(BF16)

    def window_copy(i):
        lo = i * fb // LANES * LANES
        source = x_all.at[c, block(slot), pl.ds(lo, window)]
        return source, x_win.at[slot], win_r.at[0], c * nc + i

    def x_view(side, at, k):
        wide = x_chunk + (LANES if k == x_count - 1 else 0)
        return x_all.at[side, block(at), pl.ds(k * x_chunk, wide)]

    def x_push(at, k, send, to):
        view = x_view(c, at, k)
        rcopy(view, view, send, x_r.at[at, k], to).start()

    def x_twin(at, k):
        view = x_view(c, at, k)
        rcopy(view, view, xp_s.at[0], xp_r.at[k], partner).start()

    def x_arrived(at, k):
        view = x_view(c, at, k)
        rcopy(view, view, xp_s.at[0], x_r.at[at, k], partner).wait_recv()

    gate_down = lax.rem(a, 2) == 1
    gate_up_way = lax.rem(na - 1 - a, 2) == 1

    def x_steps(d, down_line, up_line):
        for way, line, gate in ((0, down_line, gate_down), (1, up_line, gate_up_way)):
            for step in (1, 2):
                if line:
                    inside = a >= step if way == 0 else a < na - step
                    goes = inside if d == 0 and step == 1 else inside & gate
                    yield way, step, goes, dev(a - step if way == 0 else a + step, b, c)

    def at_distance(d, body):
        if d == 0:
            body(a, True, True)
            return

        @pl.when(a + d < na)
        def _():
            body(a + d, True, False)

        @pl.when(a - d >= 0)
        def _():
            body(a - d, False, True)

    def x_along(d, k, gates=True):
        if not 0 <= k < x_count:
            return

        def one(source, down_line, up_line):
            at = b * na + source

            def handle():
                if d:
                    x_arrived(at, k)
                for way, step, goes, to in x_steps(d, down_line, up_line):

                    @pl.when(goes)
                    def _():
                        x_push(at, k, xy_s.at[0], to)

                if d != 1 or k >= x_turned:
                    x_push(at, k, xy_s.at[0], across)
                x_twin(at, k)

            if d < 2:
                handle()
            else:
                gate = gate_down if down_line else gate_up_way
                pl.when(gate if gates else jnp.logical_not(gate))(handle)

        at_distance(d, one)

    def x_crossed(d, k):
        if not 0 <= k < x_count:
            return

        def one(source, down_line, up_line):
            at = (1 - b) * na + source
            x_arrived(at, k)
            if d == 0 and k < x_turned:
                for way, inside, to in ((0, a > 0, below), (1, a < na - 1, above)):

                    @pl.when(inside)
                    def _():
                        x_push(at, k, xy_s.at[0], to)

            x_twin(at, k)

        at_distance(d, one)

    def x_sent(at):
        blocks = na
        for step in (1, 2):
            blocks += (at >= step) * (1 if step == 1 else at % 2)
            blocks += (at < na - step) * (1 if step == 1 else (na - 1 - at) % 2)
            if at % 2:
                blocks += (na - 1 - at) * (at >= step)
            if (na - 1 - at) % 2:
                blocks += at * (at < na - step)
        return blocks

    s_half = s_units // 2

    def shared_project():
        loads[0].wait()
        rcopy(x_win, x_win, win_s.at[0], win_r.at[0], partner).wait_recv()
        features = x_win[...].reshape(total_rows, window)
        for side in range(2):
            for kind in range(2):
                cols = slice(kind * s_units + side * s_half, kind * s_units + (side + 1) * s_half)
                sh_part[side, :, kind * s_half : (kind + 1) * s_half] = dotted(
                    features, shared_up[:, cols]
                )
        sh_send[...] = sh_part[oc].astype(BF16)
        copy = rcopy(sh_send, sh_peer, sp_sem.at[0], sp_sem.at[1], partner)
        copy.start()
        return copy

    y_own = pl.ds(pl.multiple_of(b * y_rows, y_rows), y_rows)
    y_other = pl.ds(pl.multiple_of((1 - b) * y_rows, y_rows), y_rows)

    def shared_spread(copy):
        copy.wait()
        sh_part[0] = sh_part[c] + sh_peer[...].astype(F32)
        sh_z[...] = sh_part[0].astype(BF16).reshape(nc, pair, s_units)
        for d in range(1, nc):
            other = lax.rem(chip + d, nc)
            rcopy(
                sh_z.at[lax.rem(other, 2) * na + lax.div(other, 2)],
                sh_zr.at[d - 1],
                sz_sem.at[0],
                sz_sem.at[1],
                {"expert": other * 2 + c},
            ).start()

    others = pl.ds(0, (nc - 1) * pair)

    def shared_active():
        rcopy(sh_zr, sh_zr, sz_sem.at[0], sz_sem.at[1], partner).wait()
        total = sh_part[0, block(slot)]
        for d in range(1, nc):
            total = total + sh_zr[d - 1].astype(F32)
        sh_hidden[c, block(slot)] = (
            jax.nn.silu(total[:, :s_half]) * total[:, s_half:]
        ).astype(BF16)
        view = sh_hidden.at[c, block(slot)]
        for d in range(1, nc):
            to = {"expert": lax.rem(chip + d, nc) * 2 + c}
            rcopy(view, view, h_sem.at[0], h_sem.at[1], to).start()

    def shared_twin():
        view = sh_hidden.at[c, others]
        rcopy(view, view, h_sem.at[0], h_sem.at[1], partner).wait()
        view = sh_hidden.at[c]
        rcopy(view, view, h_sem.at[2], h_sem.at[3], partner).start()

    def shared_last():
        view = sh_hidden.at[c]
        rcopy(view, view, h_sem.at[2], h_sem.at[3], partner).wait()
        shared_down_load.wait()
        cols = dotted_nt(sh_hidden[0], shared_down[:, :s_half]) + dotted_nt(
            sh_hidden[1], shared_down[:, s_half:]
        )
        cols = cols.reshape(n, rows, fb).astype(BF16)
        for at in range(n):
            owner = 4 * (at // 2 % na) + 2 * (at // 2 // na) + at % 2
            so_send[lax.rem(owner - me + n, n)] = cols[at]
        for d in range(1, n):
            to = {"expert": lax.rem(me + d, n)}
            rcopy(so_send.at[d], so_recv.at[n - d], so_sem.at[0], so_sem.at[1], to).start()
        so_recv[0] = so_send[0]

    def shared_collect():
        view = so_recv.at[pl.ds(1, n - 1)]
        rcopy(view, view, so_sem.at[0], so_sem.at[1], partner).wait()

    def up_term(k, cols):
        at = k * x_chunk
        return dotted(x_all[0, :, at : at + x_chunk], gate_up[at : at + x_chunk, cols]) + dotted(
            x_all[1, :, at : at + x_chunk], gate_up[half + at : half + at + x_chunk, cols]
        )

    tile = min(256, units)

    def up_part(k):
        wide = x_chunk + (LANES if k == x_count - 1 else 0)
        view = x_all.at[oc, :, pl.ds(k * x_chunk, wide)]
        rcopy(view, view, xp_s.at[0], xp_r.at[k], partner).wait_recv()
        gate_up_wait(k)
        if k < x_count - 1:
            for at in range(2 * units // tile):
                cols = slice(at * tile, (at + 1) * tile)
                if k == 0:
                    up_acc[:, cols] = up_term(k, cols)
                else:
                    up_acc[:, cols] += up_term(k, cols)
            return
        for at in range(units // tile):
            gate_cols = slice(at * tile, (at + 1) * tile)
            up_cols = slice(units + at * tile, units + (at + 1) * tile)
            gate = up_term(k, gate_cols)
            up = up_term(k, up_cols)
            if k:
                gate = gate + up_acc[:, gate_cols]
                up = up + up_acc[:, up_cols]
            hidden[:, gate_cols] = (jax.nn.silu(gate) * up).astype(BF16)

    for k in range(x_count):
        x_along(0, k)
    for i in range(nc):
        source, target, recv, to = window_copy(i)

        @pl.when(to != me)
        def _():
            rcopy(source, target, win_s.at[0], recv, {"expert": to}).start()

        @pl.when(to == me)
        def _():
            pltpu.make_async_copy(source, target, recv).start()

    def gate_lag(d):
        return 3 * ((d - 1) // 2)

    def leaf_lag(d):
        return 0 if d < 2 else 3 * ((d - 2) // 2) + 3

    last_lag = leaf_lag(na - 1) + 4
    up_lag = last_lag + 2
    count = x_count + up_lag
    shared_copy = None
    for i in range(count):
        for d in range(1, na):
            x_along(d, i - gate_lag(d))
        x_crossed(0, i)
        for d in range(2, na):
            x_along(d, i - leaf_lag(d), False)
        if i == min(AT_PROJECT, count - 4):
            shared_copy = shared_project()
        if i == min(AT_ACROSS, count - 3):
            shared_spread(shared_copy)
        for d in range(1, na - 1):
            x_crossed(d, i - leaf_lag(d) - 4)
        x_crossed(na - 1, i - last_lag)
        if i >= up_lag:
            up_part(i - up_lag)

    expert = lax.div(me, group)
    codes = x_all[0, :, half:].astype(F32)
    wide = lax.broadcasted_iota(jnp.int32, (total_rows, LANES), 1) & (experts - 1)
    weight = jnp.sum(jnp.where(wide == expert, codes, 0.0), axis=1, keepdims=True)

    down_load.wait()

    def paired(j):
        return pl.ds(j, min(2, chunks - j))

    def product(side, group):
        wide = chunk * len(group)
        cols = pl.ds(pl.multiple_of(side * half + group[0] * chunk, LANES), wide)
        return dotted(hidden[...], down[:, cols]) * weight

    def send_partner(group):
        sums = product(oc, group).astype(BF16)
        for place, j in enumerate(group):
            r_p[j] = sums[:, place * chunk : (place + 1) * chunk]
        for j in group:
            rcopy(r_p.at[j], r_pr.at[j], p_s.at[0], p_r.at[j // 2], partner).start()

    def send_across(at, j, send=0):
        rcopy(r_y.at[at, j], r_yr.at[at, j], y_s.at[send], y_r.at[at, j // 2], across).start()

    far = jnp.where(2 * a >= na, 0, na - 1)
    cross_rows = block((1 - b) * na + a)

    def own_part(group):
        up_acc[:, : chunk * len(group)] = product(c, group)
        for j in group[::2]:
            view = r_pr.at[paired(j)]
            rcopy(view, view, p_s.at[0], p_r.at[j // 2], partner).wait_recv()
        for place, j in enumerate(group):
            cols = slice(place * chunk, (place + 1) * chunk)
            other = (up_acc[y_other, cols] + r_pr[j, y_other].astype(F32)).astype(BF16)
            for at in range(na):
                r_y[at, j] = other[at * pair : (at + 1) * pair]
        for place, j in enumerate(group):
            send_across(far, j)

            def beside(at, up_line, down_line):
                way, to = (1, above) if up_line else (0, below)
                rcopy(r_y.at[at, j], r_cr.at[way, j], c_s.at[0], c_r.at[way], to).start()

            if j < r_turned:
                at_distance(1, beside)
        for place, j in enumerate(group):
            cols = slice(place * chunk, (place + 1) * chunk)
            cross[j] = up_acc[cross_rows, cols] + r_pr[j, cross_rows].astype(F32)
            here = up_acc[y_own, cols] + r_pr[j, y_own].astype(F32)
            for at in range(na):
                keep[at, j] = here[at * pair : (at + 1) * pair]

    def join(j):
        for way, inside in ((1, a > 0), (0, a < na - 1)) if j < r_turned else ():

            @pl.when(inside)
            def _():
                if j == 0:
                    view = r_cr.at[way, pl.ds(0, r_turned)]
                    rcopy(view, view, c_s.at[0], c_r.at[way], across).wait_recv()
                cross[j] = cross[j] + r_cr[way, j].astype(F32)

        r_y[a, j] = cross[j].astype(BF16)
        send_across(a, j)

    def y_arrived(at, j):
        if j % 2 == 0:
            view = r_yr.at[at, paired(j)]
            rcopy(view, view, y_s.at[0], y_r.at[at, j // 2], across).wait_recv()

    def z_place(step, place):
        if step == 1 or na > 4:
            return (step - 1) * (na + 1) + place
        return na + 1 + (place is na)

    def z_add(step, place, at, j):
        index = z_place(step, place)
        if j % 2 == 0:
            view = r_zr.at[index, paired(j)]
            rcopy(view, view, z_s.at[0], z_r.at[index, j // 2], across).wait_recv()
        keep[at, j] = keep[at, j] + r_zr[index, j].astype(F32)

    def gate_even(up_line):
        return lax.rem(na - 1 - a if up_line else a, 2) == 0

    def leaf(up_line):
        return jnp.logical_not(gate_even(up_line))

    def z_pass(d, j, only=None):
        def one(at, up_line, down_line):
            if only is None:
                forward(at, up_line)
            else:
                pl.when(only(up_line))(lambda: forward(at, up_line))

        def forward(at, up_line):
            if d > 1 or j >= r_turned:
                y_arrived(at, j)
                keep[at, j] = keep[at, j] + r_yr[at, j].astype(F32)
            for step in (1, 2):
                if d + step < na:

                    @pl.when(gate_even(up_line) & (a >= step if up_line else a < na - step))
                    def _():
                        z_add(step, at, at, j)

            r_z[at, j] = keep[at, j].astype(BF16)
            last = na if not up_line else at

            def send(hop, place):
                to = dev(a + hop if up_line else a - hop, b, c)
                index = z_place(hop, place)
                rcopy(
                    r_z.at[at, j], r_zr.at[index, j], z_s.at[0], z_r.at[index, j // 2], to
                ).start()

            if d == 1:
                send(1, last)
            else:
                even = gate_even(up_line)
                pl.when(even)(lambda: send(2, last if d == 2 else at))
                pl.when(jnp.logical_not(even))(lambda: send(1, at))

        at_distance(d, one)

    def collect(j):
        y_arrived(a, j)
        keep[a, j] = keep[a, j] + r_yr[a, j].astype(F32)
        for step in (1, 2):
            for place, inside, up_line in ((a, a >= step, True), (na, a < na - step, False)):
                if step == 2:
                    inside = inside & gate_even(up_line)

                @pl.when(inside)
                def _():
                    z_add(step, place, a, j)

        total = keep[a, j]
        res[0, j] = total[:rows]
        res[1, j] = total[rows:]
        rcopy(res.at[oc, j], res_r.at[j], l_s.at[0], l_r.at[j // 2], partner).start()

    groups = [tuple(range(j, min(j + GROUPED, chunks))) for j in range(0, chunks, GROUPED)]
    send_partner(groups[0])
    for at, group in enumerate(groups):
        if at + 1 < len(groups):
            send_partner(groups[at + 1])
        if at == len(groups) - 1:
            shared_active()
        own_part(group)
        for j in group:
            if j < r_turned:
                z_pass(1, j, leaf)
    for d in range(na - 2, 1, -1):

        def send_rest(at, up_line, down_line):
            @pl.when(at != far)
            def _():
                for j in range(chunks):
                    send_across(at, j)

        at_distance(d, send_rest)
    for j in range(r_turned, chunks):
        at_distance(1, lambda at, up_line, down_line: send_across(at, j, 1))
    for j in range(chunks):
        join(j)
    for d in range(na - 1, 2, -1):
        for j in range(chunks):
            z_pass(d, j)
    if na > 2:
        for j in range(chunks):
            z_pass(2, j, leaf)
    shared_twin()
    if na > 2:
        for j in range(chunks):
            z_pass(2, j, gate_even)
    shared_last()
    for j in range(chunks):
        z_pass(1, j, gate_even if j < r_turned else None)
    for j in range(chunks):
        collect(j)
    shared_collect()
    for j in range(chunks):
        if j % 2 == 0:
            view = res_r.at[paired(j)]
            rcopy(view, view, l_s.at[0], l_r.at[j // 2], partner).wait_recv()
        own_cols = pl.ds(pl.multiple_of(c * half + j * chunk, LANES), chunk)
        other_cols = pl.ds(pl.multiple_of(oc * half + j * chunk, LANES), chunk)
        acc[:, own_cols] = res[c, j]
        acc[:, other_cols] = res_r[j]
    for at in range(n):
        cols = slice(at * fb, (at + 1) * fb)
        acc[:, cols] = acc[:, cols] + so_recv[lax.rem(at - me + n, n)].astype(F32)
    row_of = lax.broadcasted_iota(jnp.int32, (rows_dev, width), 0)
    for step in range(steps):
        update = acc[step * rows_dev : (step + 1) * rows_dev]
        update = jnp.where(row_of < live_ref[:, step : step + 1], update, 0.0)
        out_ref[step] = (tokens_ref[step].astype(F32) + update).astype(BF16)
    @pl.when(lax.div(me, nc) == c)
    def _():
        view = x_win.at[pl.ds(0, nc - 1)]
        rcopy(view, view, win_s.at[0], win_r.at[0], partner).wait_send()

    @pl.when(lax.div(me, nc) != c)
    def _():
        rcopy(x_win, x_win, win_s.at[0], win_r.at[0], partner).wait_send()

    for at in range(na):

        @pl.when(a == at)
        def _():
            left = x_sent(at)
            while left:
                some = min(left, nc)
                view = x_all.at[c, pl.ds(0, some * pair)]
                rcopy(view, view, xy_s.at[0], x_r.at[0, 0], partner).wait_send()
                left -= some

    view = x_all.at[c]
    rcopy(view, view, xp_s.at[0], xp_r.at[0], partner).wait_send()
    rcopy(r_p, r_pr, p_s.at[0], p_r.at[0], partner).wait_send()
    for at in range(na):
        beside = (at > 0) + (at < na - 1)

        @pl.when(a == at)
        def _():
            if r_turned:
                view = r_y.at[pl.ds(0, beside), pl.ds(0, r_turned)]
                rcopy(view, view, c_s.at[0], c_r.at[0], across).wait_send()
            view = r_y.at[pl.ds(0, na - beside)]
            rcopy(view, view, y_s.at[0], y_r.at[0, 0], across).wait_send()
            if r_turned < chunks:
                view = r_y.at[pl.ds(0, beside), pl.ds(0, chunks - r_turned)]
                rcopy(view, view, y_s.at[1], y_r.at[0, 0], across).wait_send()

    view = r_z.at[pl.ds(0, na - 1)]
    rcopy(view, view, z_s.at[0], z_r.at[0, 0], across).wait_send()
    view = res.at[oc]
    rcopy(view, res_r, l_s.at[0], l_r.at[0], partner).wait_send()


def per_device(
    tokens,
    live_rows,
    expert_ids,
    gate_weights,
    norm_gain,
    expert_gate_up,
    expert_down,
    shared_gate_up,
    shared_down,
):
    step_count, row_count, model_width = tokens.shape
    n = lax.axis_size("expert")
    group = n // EXPERTS
    units = expert_down.shape[2]
    fb, s_wide = shared_gate_up.shape[1:]
    s_units = s_wide // 2
    nc = n // 2
    na = nc // 2
    half = model_width // 2
    rows = step_count * row_count
    pair = 2 * rows
    total = nc * pair
    y_rows = na * pair
    wide = half + LANES
    chunk = next(size for size in (512, 256, 128) if half % size == 0)
    chunks = half // chunk
    span = next(size for size in (128, 64, 32, 16) if fb % size == 0)
    window = -(-(fb + LANES - span) // LANES) * LANES
    dma = pltpu.SemaphoreType.DMA
    vmem = pltpu.VMEM
    whole = pl.BlockSpec(memory_space=pltpu.VMEM)
    anywhere = pl.BlockSpec(memory_space=pl.ANY)
    x_chunk = chunk if nc <= EXPERTS else half
    x_count = half // x_chunk
    x_turned = min(X_TURNED, x_count)
    r_turned = min(R_TURNED, chunks)
    pairs = (chunks + 1) // 2
    z_places = 2 * na + 2 if na > 4 else na + 3
    return pl.pallas_call(
        functools.partial(layer_kernel, n, EXPERTS, group, chunk, window, x_chunk, x_turned, r_turned),
        out_shape=jax.ShapeDtypeStruct(tokens.shape, BF16),
        in_specs=[whole] * 5 + [anywhere] * 4,
        out_specs=whole,
        scratch_shapes=[
            vmem((rows, model_width), F32),
            vmem((2, rows, wide), F32),
            vmem((rows, wide), F32),
            vmem((2, total, wide), BF16),
            vmem((nc, pair, window), BF16),
            vmem((model_width, 2 * units), BF16),
            vmem((units, model_width), BF16),
            vmem((window, s_wide), BF16),
            vmem((fb, s_units), BF16),
            vmem((total, max(2 * units, GROUPED * chunk)), F32),
            vmem((total, units), BF16),
            vmem((2, total, s_units), F32),
            vmem((total, s_units), BF16),
            vmem((total, s_units), BF16),
            vmem((nc, pair, s_units), BF16),
            vmem((nc - 1, pair, s_units), BF16),
            vmem((2, total, s_units // 2), BF16),
            vmem((n, rows, fb), BF16),
            vmem((n, rows, fb), BF16),
            vmem((chunks, total, chunk), BF16),
            vmem((chunks, total, chunk), BF16),
            vmem((na, chunks, pair, chunk), BF16),
            vmem((na, chunks, pair, chunk), BF16),
            vmem((na, chunks, pair, chunk), BF16),
            vmem((z_places, chunks, pair, chunk), BF16),
            vmem((2, chunks, pair, chunk), BF16),
            vmem((chunks, pair, chunk), F32),
            vmem((na, chunks, pair, chunk), F32),
            vmem((2, chunks, rows, chunk), F32),
            vmem((chunks, rows, chunk), F32),
            dma((3 + x_count,)),
            dma((2,)),
            dma((1,)),
            dma((1,)),
            dma((1,)),
            dma((1,)),
            dma((nc, x_count)),
            dma((x_count,)),
            dma((4,)),
            dma((2,)),
            dma((2,)),
            dma((2,)),
            dma((1,)),
            dma((pairs,)),
            dma((1,)),
            dma((2,)),
            dma((2,)),
            dma((na, pairs)),
            dma((1,)),
            dma((z_places, pairs)),
            dma((1,)),
            dma((pairs,)),
        ],
        compiler_params=pltpu.CompilerParams(
            collective_id=0, has_side_effects=True, vmem_limit_bytes=67_043_328
        ),
    )(
        tokens,
        live_rows.T,
        expert_ids,
        gate_weights,
        norm_gain,
        expert_gate_up,
        expert_down,
        shared_gate_up,
        jnp.swapaxes(shared_down, 1, 2),
    )


def solution(mesh):
    placed = (
        P(None, ("parts", "expert"), None),
        P(None, ("parts", "expert")),
        P(None, None, ("parts", "expert"), None),
        P(None, None, ("parts", "expert"), None),
        P(),
        P(None, "expert", None, None),
        P(None, "expert", None, None),
        P(None, "expert", None),
        P(None, None, "expert"),
    )
    return jax.shard_map(
        per_device,
        mesh=mesh,
        in_specs=placed,
        out_specs=P(None, ("parts", "expert"), None),
        check_vma=False,
    )
```
